128 devices in a mesh: gz: 2 (over core), gx: 16 (over z, y), gy: 4 (over x).
Axes of the slice: x: 4, y: 4, z: 4, core: 2. Of those that a mesh axis runs over, the one named last changes fastest.
Arguments:
- pair_repr: bfloat16 [8, 384, 384, 128], P('gz', 'gx', 'gy'), may hold values from -9 to 9
- seq_lengths: int32 [8], replicated, may hold values from 96 to 384
- weight_in: bfloat16 [128, 640], replicated, may hold values from -0.5 to 0.5
- weight_out: bfloat16 [128, 128], replicated, may hold values from -0.5 to 0.5
Outputs:
- updated: bfloat16 [8, 384, 384, 128], P('gz', 'gx', 'gy')
- magnitude: float32 [], replicated
The draws below stay inside these ranges and needn't reach their ends.
All inputs are finite; a program needn't handle non-finite values.
Results may differ from the reference program's by a relative error of at most 0.0034.
Values may be sent and summed in bfloat16 or wider, within the bound.
A program may use at most 320 MiB of HBM per device.

```python
import math
import jax
import jax.numpy as jnp
from jax import lax

C = 128
CH = 128
N = 384
BATCH = 8


def draw_pair_repr(key, part):
    split_keys = jax.random.split(jax.random.fold_in(key, 17), 3)
    row_ramp = 0.5 + jnp.arange(N, dtype=jnp.float32) / N
    row_scale = jnp.exp(jax.random.uniform(split_keys[1], (BATCH, N, 1, 1), jnp.float32, math.log(0.7), math.log(1.4)))
    col_scale = jnp.exp(jax.random.uniform(split_keys[2], (BATCH, 1, N, 1), jnp.float32, math.log(0.7), math.log(1.4)))
    base_values = jnp.clip(jax.random.normal(split_keys[0], (BATCH, N, N, C), jnp.float32), -3.0, 3.0)
    values = base_values * row_ramp[None, :, None, None] * row_scale * col_scale
    return values.astype(jnp.bfloat16)


def with_ends(array, key, least, top_value):
    longest = array.shape.index(max(array.shape))
    spots = []
    for shift in (0, 1):
        where = [jax.random.randint(jax.random.fold_in(key, axis), (), 0, length) for axis, length in enumerate(array.shape)]
        where[longest] = (where[longest] + shift) % array.shape[longest]
        spots.append(tuple(where))
    return array.at[spots[0]].set(least).at[spots[1]].set(top_value)


def noise(rng, extent, scale, most, held_as=jnp.bfloat16):
    array = scale * jax.random.normal(rng, extent, jnp.float32)
    return jnp.clip(array, min=-most, max=most).astype(held_as)


def setup_inputs(seed: int = 0) -> dict:
    seeds = jax.random.split(jax.random.key(seed), 5)
    pair_repr = draw_pair_repr(jax.random.fold_in(seeds[4], 71), 0)
    seq_lengths = with_ends(jax.random.randint(seeds[1], (BATCH,), N // 4, N + 1), jax.random.fold_in(seeds[1], 1), N // 4, N).astype(jnp.int32)
    weight_in = noise(seeds[2], (C, 4 * CH + C), C ** -0.5, 0.5)
    weight_out = noise(seeds[3], (CH, C), CH ** -0.5, 0.5)
    return dict(pair_repr=pair_repr, seq_lengths=seq_lengths, weight_in=weight_in, weight_out=weight_out)


def layer_norm(values):
    mean_value = lax.optimization_barrier(jnp.mean(values, axis=-1, keepdims=True))
    centered = values - mean_value
    variance = lax.optimization_barrier(jnp.mean(centered * centered, axis=-1, keepdims=True))
    return centered * lax.rsqrt(variance + 1e-05)

def reference(pair_repr, seq_lengths, weight_in, weight_out):

    def one_tensor(inputs):
        pair_one, length_one = inputs
        positions = jnp.arange(N, dtype=jnp.int32)
        row_live = (positions < length_one).astype(jnp.float32)
        pair_mask = (row_live[:, None] * row_live[None, :])[:, :, None]
        normed = layer_norm(pair_one.astype(jnp.float32)).astype(jnp.bfloat16)
        proj = jnp.dot(normed.reshape(N * N, C), weight_in, preferred_element_type=jnp.float32).reshape(N, N, 4 * CH + C)
        left_proj = (pair_mask * jax.nn.sigmoid(proj[..., CH:2 * CH]) * proj[..., :CH]).astype(jnp.bfloat16)
        right_proj = (pair_mask * jax.nn.sigmoid(proj[..., 3 * CH:4 * CH]) * proj[..., 2 * CH:3 * CH]).astype(jnp.bfloat16)
        gate_values = jax.nn.sigmoid(proj[..., 4 * CH:])
        triangle = jnp.einsum('kic,kjc->ijc', left_proj.astype(jnp.float32), right_proj.astype(jnp.float32), precision=lax.Precision.HIGHEST)
        tri_normed = layer_norm(triangle).astype(jnp.bfloat16)
        projected = jnp.dot(tri_normed.reshape(N * N, CH), weight_out, preferred_element_type=jnp.float32).reshape(N, N, C)
        update = pair_mask * gate_values * projected
        return (pair_one.astype(jnp.float32) + update).astype(jnp.bfloat16)
    updated = lax.map(one_tensor, (pair_repr, seq_lengths))
    entry_count = float(BATCH * N * N * C)
    magnitude = jnp.sum(jnp.abs(updated.astype(jnp.float32))) / entry_count
    return (updated, magnitude)
```

```python
import jax
import jax.numpy as jnp
from jax import lax
from jax.experimental import pallas as pl
from jax.experimental.pallas import tpu as pltpu
from jax.sharding import Mesh
from jax.sharding import PartitionSpec as P

AXES = ("gz", "gx_0", "gx_1", "gy")
GX = ("gx_0", "gx_1")
MESH_ID = pl.DeviceIdType.MESH
F32 = jnp.float32
BF16 = jnp.bfloat16
EPS = 1e-05


def dot(a, b, ca, cb):
    return lax.dot_general(a, b, (((ca,), (cb,)), ((), ())), preferred_element_type=F32)


def kernel(
    entries,
    lens, pair, w_in, w_out,
    updated, magnitude,
    s_l, s_r, d_l, d_r, turned, s_t, d_t, normed, gates, w_proj, w_gate, w_last, s_mag, d_mag,
    send_l, send_r, send_t, send_m, recv_l, recv_r, recv_t, recv_m,
):
    core, z, y, x = (lax.axis_index(a) for a in AXES)
    gx = z * 4 + y
    me = gx * 4 + x

    barrier = pltpu.get_barrier_semaphore()

    def greet(r, carry):
        other = lax.rem(core * 64 + me + r, 128)
        pl.semaphore_signal(
            barrier,
            inc=1,
            device_id=(other // 64, other // 16 % 4, other // 4 % 4, other % 4),
            device_id_type=MESH_ID,
        )
        return carry

    lax.fori_loop(1, 128, greet, 0)

    row2 = lax.broadcasted_iota(jnp.int32, (256, 128), 0)
    col2 = lax.broadcasted_iota(jnp.int32, (256, 128), 1)
    twice = (row2 // 2 == col2).astype(BF16)
    even = row2 % 2 == 0
    for kind in range(4):
        part = dot(twice, w_in[:, kind * 128 : (kind + 1) * 128], 1, 1)
        part = part * (0.5 if kind % 2 else 1.0)
        rows = pl.ds(kind * 256, 256)
        w_proj[rows, 0:128] = jnp.where(even, part, 0.0).astype(BF16)
        w_proj[rows, 128:256] = jnp.where(even, 0.0, part).astype(BF16)
    part = dot(twice, w_out[...], 1, 0)
    w_last[:, 0:128] = jnp.where(even, part, 0.0).astype(BF16)
    w_last[:, 128:256] = jnp.where(even, 0.0, part).astype(BF16)
    half_gate = w_in[:, 512:640] * 0.5
    nothing = jnp.zeros((128, 128), BF16)
    w_gate[0:128, 0:128] = half_gate.astype(BF16)
    w_gate[0:128, 128:256] = nothing
    w_gate[128:256, 0:128] = nothing
    w_gate[128:256, 128:256] = half_gate.astype(BF16)

    my_len = [lens[core * 4 + b] for b in range(4)]
    lane = lax.broadcasted_iota(jnp.int32, (8, 128), 1)
    sub = lax.broadcasted_iota(jnp.int32, (8, 128), 0)
    group = lane // 32
    len_lane = jnp.where(
        group == 0,
        my_len[0],
        jnp.where(group == 1, my_len[1], jnp.where(group == 2, my_len[2], my_len[3])),
    )
    s_l2 = s_l.reshape(36, 256, 128)
    s_r2 = s_r.reshape(36, 256, 128)
    d_l2 = d_l.reshape(24, 384, 128)
    d_r2 = d_r.reshape(24, 384, 128)
    d_t2 = d_t.reshape(36, 256, 128)

    def pair_rows(row, third):
        return jnp.concatenate(
            [pair[b, row, third * 32 : (third + 1) * 32, :] for b in range(4)], axis=0
        )

    def normalize(third):
        def body(q, carry):
            halves = []
            for parity in range(2):
                v = pair_rows(2 * q + parity, third).astype(F32)
                mean_value = jnp.sum(v, axis=1, keepdims=True) * (1.0 / 128)
                v = v - mean_value
                variance = jnp.sum(v * v, axis=1, keepdims=True) * (1.0 / 128)
                halves.append((v * lax.rsqrt(variance + EPS)).astype(BF16))
            normed[third * 12 + q] = jnp.concatenate(halves, axis=1)
            return carry

        lax.fori_loop(0, 12, body, 0)

    def project(third, first, store):
        def body(q, carry):
            out = dot(w_proj[first : first + 512, :], normed[third * 12 + q], 1, 1)
            i_lane = x * 96 + third * 32 + lane % 32
            k_sub = gx * 24 + 2 * q + sub % 2
            half_mask = jnp.where((i_lane < len_lane) & (k_sub < len_lane), 0.5, 0.0)
            value = out[0:256].reshape(32, 8, 128) * half_mask[None]
            gate = jnp.tanh(out[256:512]).reshape(32, 8, 128) + 1.0
            store[third * 12 + q] = (value * gate).reshape(256, 128).astype(BF16)
            return carry

        lax.fori_loop(0, 12, body, 0)

    def other_of(r):
        off = lax.rem(r * 27, 64)
        oz = lax.rem(z + off // 16, 4)
        oy = lax.rem(y + off // 4 % 4, 4)
        ox = lax.rem(x + off % 4, 4)
        return oz, oy, ox

    def send_part(third, source, target, send_sem, recv_sem):
        def body(r, carry):
            oz, oy, ox = other_of(r)
            channel = (oz * 16 + oy * 4 + ox) * 2
            for c in range(2):
                pltpu.make_async_remote_copy(
                    src_ref=source.at[third, :, channel + c],
                    dst_ref=target.at[c, third, x, pl.ds(gx * 12, 12)],
                    send_sem=send_sem,
                    recv_sem=recv_sem.at[third],
                    device_id=(core, oz, oy, ox),
                    device_id_type=MESH_ID,
                ).start()
            return carry

        lax.fori_loop(1, 64, body, 0)
        for c in range(2):
            target[c, third, x, pl.ds(gx * 12, 12)] = source[third, :, me * 2 + c]

    def wait_part(sem):
        part = d_t.at[0, :, pl.ds(0, 126)]
        pltpu.make_async_copy(part, part, sem).wait()

    for third in range(3):
        normalize(third)
        project(third, 0, s_l2)
        if third == 0:
            pl.semaphore_wait(barrier, 127)
        send_part(third, s_l, d_l, send_l, recv_l)
    for third in range(3):
        project(third, 512, s_r2)
        send_part(third, s_r, d_r, send_r, recv_r)

    def gate_body(third):
        def body(q, carry):
            out = dot(normed[third * 12 + q], w_gate[...], 1, 0)
            parts = []
            for b in range(4):
                j_row = x * 96 + third * 32 + lax.broadcasted_iota(jnp.int32, (32, 256), 0)
                i_lane = gx * 24 + 2 * q + lax.broadcasted_iota(jnp.int32, (32, 256), 1) // 128
                live = (j_row < my_len[b]) & (i_lane < my_len[b])
                half = out[b * 32 : (b + 1) * 32]
                parts.append(jnp.where(live, jnp.tanh(half) * 0.5 + 0.5, 0.0))
            gates[third * 12 + q] = jnp.concatenate(parts, axis=0)
            return carry

        lax.fori_loop(0, 12, body, 0)

    for third in range(3):
        gate_body(third)

    for third in range(3):
        wait_part(recv_l.at[third])

        def turn(n, carry):
            c = n // 4
            col = lax.rem(n, 4)
            block = d_l2[c * 12 + third * 4 + col]
            turned[n, third * 128 : (third + 1) * 128, :] = block.T
            return carry

        lax.fori_loop(0, 8, turn, 0)

    lane4 = lax.broadcasted_iota(jnp.int32, (32, 512), 1) % 128 // 32

    def multiply(third):
        def body(r, carry):
            block = lax.rem(z + r, 4)
            for c in range(2):
                right = jnp.concatenate(
                    [d_r2[c * 12 + third * 4 + col] for col in range(4)], axis=1
                )
                out = dot(turned[c * 4 + block], right, 1, 0)
                rows = []
                for t in range(3):
                    g = [out[t * 128 + b * 32 : t * 128 + (b + 1) * 32] for b in range(4)]
                    rows.append(
                        jnp.where(
                            lane4 == 0,
                            g[0],
                            jnp.where(lane4 == 1, g[1], jnp.where(lane4 == 2, g[2], g[3])),
                        )
                    )
                full = jnp.concatenate(rows, axis=0)
                for piece in range(4):
                    for col in range(4):
                        s_t[third, block * 4 + piece, col, :, c] = (
                            full[piece * 24 : (piece + 1) * 24, col * 128 : (col + 1) * 128]
                            .astype(BF16)
                            .reshape(12, 2, 128)
                        )

            def send_one(n, inner):
                oy = lax.rem(y + n // 4, 4)
                ox = lax.rem(x + n, 4)
                pltpu.make_async_remote_copy(
                    src_ref=s_t.at[third, block * 4 + oy, ox],
                    dst_ref=d_t.at[third, :, pl.ds(me * 2, 2)],
                    send_sem=send_t,
                    recv_sem=recv_t.at[third],
                    device_id=(core, block, oy, ox),
                    device_id_type=MESH_ID,
                ).start()
                return inner

            lax.fori_loop(jnp.where(r == 4, 1, 0), 16, send_one, 0)
            return carry

        lax.fori_loop(1, 5, body, 0)
        d_t[third, :, pl.ds(me * 2, 2)] = s_t[third, gx, x]

    def finish(third, total):
        def body(q, total):
            v = d_t2[third * 12 + q].astype(F32).reshape(32, 8, 128)

            def over_channels(array):
                s = jnp.sum(array, axis=0)
                s = s + pltpu.roll(s, 4, 0)
                s = s + pltpu.roll(s, 2, 0)
                return s * (1.0 / 128)

            v = v - over_channels(v)[None]
            v = v * lax.rsqrt(over_channels(v * v) + EPS)[None]
            out = dot(v.reshape(256, 128).astype(BF16), w_last[...], 0, 0)
            change = out * gates[third * 12 + q]
            for parity in range(2):
                new = pair_rows(2 * q + parity, third).astype(F32)
                new = (new + change[:, parity * 128 : (parity + 1) * 128]).astype(BF16)
                for b in range(4):
                    updated[b, 2 * q + parity, third * 32 : (third + 1) * 32, :] = new[
                        b * 32 : (b + 1) * 32
                    ]
                total = total + jnp.sum(jnp.abs(new.astype(F32)).reshape(16, 8, 128), axis=0)
            return total

        return lax.fori_loop(0, 12, body, total)

    for third in range(3):
        wait_part(recv_r.at[third])
        multiply(third)
    total = jnp.zeros((8, 128), F32)
    for third in range(3):
        wait_part(recv_t.at[third])
        total = finish(third, total)

    flat = core * 64 + me
    s_mag[...] = jnp.sum(total, axis=0, keepdims=True)
    d_mag[flat] = jnp.sum(total, axis=0, keepdims=True)

    def tell(r, carry):
        other = lax.rem(flat + r, 128)
        pltpu.make_async_remote_copy(
            src_ref=s_mag,
            dst_ref=d_mag.at[flat],
            send_sem=send_m,
            recv_sem=recv_m,
            device_id=(other // 64, other // 16 % 4, other // 4 % 4, other % 4),
            device_id_type=MESH_ID,
        ).start()
        return carry

    lax.fori_loop(1, 128, tell, 0)
    for _ in range(3):
        wait_part(send_l)
        wait_part(send_r)
        wait_part(send_t)
    rest = d_mag.at[pl.ds(0, 127)]
    pltpu.make_async_copy(rest, rest, send_m).wait()
    pltpu.make_async_copy(rest, rest, recv_m).wait()
    everyone = jnp.sum(d_mag[...], axis=0)
    magnitude[...] = jnp.sum(everyone, axis=1, keepdims=True) * (1.0 / entries)


def per_device(entries, pair_repr, seq_lengths, weight_in, weight_out):
    vmem = pl.BlockSpec(memory_space=pltpu.VMEM)
    dma = pltpu.SemaphoreType.DMA
    updated, magnitude = pl.pallas_call(
        lambda *refs: kernel(entries, *refs),
        out_shape=(
            jax.ShapeDtypeStruct(pair_repr.shape, BF16),
            jax.ShapeDtypeStruct((1, 1), F32),
        ),
        in_specs=[pl.BlockSpec(memory_space=pltpu.SMEM), vmem, vmem, vmem],
        out_specs=(vmem, vmem),
        scratch_shapes=[
            pltpu.VMEM((3, 12, 128, 2, 128), BF16),
            pltpu.VMEM((3, 12, 128, 2, 128), BF16),
            pltpu.VMEM((2, 3, 4, 192, 2, 128), BF16),
            pltpu.VMEM((2, 3, 4, 192, 2, 128), BF16),
            pltpu.VMEM((8, 384, 384), BF16),
            pltpu.VMEM((3, 16, 4, 12, 2, 2, 128), BF16),
            pltpu.VMEM((3, 12, 128, 2, 128), BF16),
            pltpu.VMEM((36, 128, 256), BF16),
            pltpu.VMEM((36, 128, 256), F32),
            pltpu.VMEM((1024, 256), BF16),
            pltpu.VMEM((256, 256), BF16),
            pltpu.VMEM((256, 256), BF16),
            pltpu.VMEM((1, 128), F32),
            pltpu.VMEM((128, 1, 128), F32),
            dma,
            dma,
            dma,
            dma,
            dma((3,)),
            dma((3,)),
            dma((3,)),
            dma,
        ],
        compiler_params=pltpu.CompilerParams(
            collective_id=0, has_side_effects=True, vmem_limit_bytes=56 * 2**20
        ),
        name="triangle",
    )(seq_lengths, pair_repr, weight_in, weight_out)
    return updated, magnitude.reshape(())


def solution(mesh):
    finer = Mesh(mesh.devices.reshape(mesh.shape["gz"], 4, 4, mesh.shape["gy"]), AXES)
    entries = float(8 * 384 * 384 * 128)
    return jax.shard_map(
        lambda *args: per_device(entries, *args),
        mesh=finer,
        in_specs=(P("gz", GX, "gy", None), P(), P(), P()),
        out_specs=(P("gz", GX, "gy", None), P()),
        check_vma=False,
    )
```

```python
import jax
import jax.numpy as jnp
from jax import lax
from jax.experimental import pallas as pl
from jax.experimental.pallas import tpu as pltpu
from jax.sharding import Mesh
from jax.sharding import PartitionSpec as P

AXES = ("gz", "gx_0", "gx_1", "gy")
GX = ("gx_0", "gx_1")
MESH_ID = pl.DeviceIdType.MESH
F32 = jnp.float32
BF16 = jnp.bfloat16
EPS = 1e-05
U_NORM = 3
U_PROJ = 2
U_GATE = 2
U_LAST = 2


def steps(count, unroll, body, carry):
    def several(n, carry):
        for u in range(unroll):
            carry = body(n * unroll + u, carry)
        return carry

    return lax.fori_loop(0, count // unroll, several, carry)


def dot(a, b, ca, cb):
    return lax.dot_general(a, b, (((ca,), (cb,)), ((), ())), preferred_element_type=F32)


def kernel(
    entries,
    lens, pair_hbm, w_in_hbm, w_out_hbm,
    updated, magnitude,
    pair, w_in, w_out,
    s_l, s_r, d_l, d_r, turned, s_t, d_t, normed, gates, w_proj, w_gate, w_last,
    s_plane, d_plane, s_all, d_all,
    send_l, send_r, send_t, send_m, recv_l, recv_r, recv_t, recv_plane, recv_all,
    fetched,
):
    core, z, y, x = (lax.axis_index(a) for a in AXES)
    gx = z * 4 + y
    me = gx * 4 + x

    def columns(third):
        return pl.ds(third * 32, 32)

    fetch = [
        pltpu.make_async_copy(w_in_hbm, w_in, fetched.at[3]),
        pltpu.make_async_copy(
            pair_hbm.at[:, :, columns(0)], pair.at[:, :, columns(0)], fetched.at[0]
        ),
        pltpu.make_async_copy(w_out_hbm, w_out, fetched.at[4]),
        pltpu.make_async_copy(
            pair_hbm.at[:, :, columns(1)], pair.at[:, :, columns(1)], fetched.at[1]
        ),
        pltpu.make_async_copy(
            pair_hbm.at[:, :, columns(2)], pair.at[:, :, columns(2)], fetched.at[2]
        ),
    ]
    for copy in fetch:
        copy.start()

    barrier = pltpu.get_barrier_semaphore()
    zs = [lax.rem(z + n, 4) for n in range(4)]
    ys = [lax.rem(y + n, 4) for n in range(4)]
    xs = [lax.rem(x + n, 4) for n in range(4)]

    def greet(device):
        pl.semaphore_signal(barrier, inc=1, device_id=device, device_id_type=MESH_ID)

    for dz in range(4):
        for dy in range(4):
            for dx in range(4):
                if dz or dy or dx:
                    greet((core, zs[dz], ys[dy], xs[dx]))
        greet((1 - core, zs[dz], y, x))

    row2 = lax.broadcasted_iota(jnp.int32, (256, 128), 0)
    col2 = lax.broadcasted_iota(jnp.int32, (256, 128), 1)
    twice = (row2 // 2 == col2).astype(BF16)
    even = row2 % 2 == 0
    fetch[0].wait()
    for kind in range(4):
        part = dot(twice, w_in[:, kind * 128 : (kind + 1) * 128], 1, 1)
        part = part * (0.5 if kind % 2 else 1.0)
        rows = pl.ds(kind * 256, 256)
        w_proj[rows, 0:128] = jnp.where(even, part, 0.0).astype(BF16)
        w_proj[rows, 128:256] = jnp.where(even, 0.0, part).astype(BF16)

    my_len = [lens[core * 4 + b] for b in range(4)]
    lane = lax.broadcasted_iota(jnp.int32, (8, 128), 1)
    sub = lax.broadcasted_iota(jnp.int32, (8, 128), 0)
    group = lane // 32
    len_lane = jnp.where(
        group == 0,
        my_len[0],
        jnp.where(group == 1, my_len[1], jnp.where(group == 2, my_len[2], my_len[3])),
    )
    s_l2 = s_l.reshape(36, 256, 128)
    s_r2 = s_r.reshape(36, 256, 128)
    d_l2 = d_l.reshape(24, 384, 128)
    d_r2 = d_r.reshape(24, 384, 128)
    d_t2 = d_t.reshape(36, 256, 128)

    def pair_rows(row, third):
        return jnp.concatenate(
            [pair[b, row, third * 32 : (third + 1) * 32, :] for b in range(4)], axis=0
        )

    def normalize(third):
        def body(q, carry):
            halves = []
            for parity in range(2):
                v = pair_rows(2 * q + parity, third).astype(F32)
                mean_value = jnp.sum(v, axis=1, keepdims=True) * (1.0 / 128)
                v = v - mean_value
                variance = jnp.sum(v * v, axis=1, keepdims=True) * (1.0 / 128)
                halves.append((v * lax.rsqrt(variance + EPS)).astype(BF16))
            normed[third * 12 + q] = jnp.concatenate(halves, axis=1)
            return carry

        steps(12, U_NORM, body, 0)

    def project(third, first, store):
        def body(q, carry):
            out = dot(w_proj[first : first + 512, :], normed[third * 12 + q], 1, 1)
            i_lane = x * 96 + third * 32 + lane % 32
            k_sub = gx * 24 + 2 * q + sub % 2
            half_mask = jnp.where((i_lane < len_lane) & (k_sub < len_lane), 0.5, 0.0)
            value = out[0:256].reshape(32, 8, 128) * half_mask[None]
            gate = jnp.tanh(out[256:512]).reshape(32, 8, 128) + 1.0
            store[third * 12 + q] = (value * gate).reshape(256, 128).astype(BF16)
            return carry

        steps(12, U_PROJ, body, 0)

    def to_others(send):
        def body(n, carry):
            oz = lax.rem(z + n, 4)
            oy = lax.rem(y + n // 4, 4)
            for dx in range(4):
                send(lax.rem(oz + dx, 4), lax.rem(oy + dx, 4), xs[dx])
            return carry

        lax.fori_loop(1, 16, body, 0)
        for dx in range(1, 4):
            send(zs[dx], ys[dx], xs[dx])

    def send_part(third, source, target, send_sem, recv_sem):
        def send(oz, oy, ox):
            channel = (oz * 16 + oy * 4 + ox) * 2
            for c in range(2):
                pltpu.make_async_remote_copy(
                    src_ref=source.at[third, :, channel + c],
                    dst_ref=target.at[c, third, x, pl.ds(gx * 12, 12)],
                    send_sem=send_sem,
                    recv_sem=recv_sem.at[third],
                    device_id=(core, oz, oy, ox),
                    device_id_type=MESH_ID,
                ).start()

        to_others(send)
        for c in range(2):
            target[c, third, x, pl.ds(gx * 12, 12)] = source[third, :, me * 2 + c]

    def wait_part(sem, rows=12):
        part = d_t.at[0, pl.ds(0, rows), pl.ds(0, 126)]
        pltpu.make_async_copy(part, part, sem).wait()

    for third in range(3):
        fetch[(1, 3, 4)[third]].wait()
        normalize(third)
        project(third, 0, s_l2)
        if third == 0:
            pl.semaphore_wait(barrier, 67)
        send_part(third, s_l, d_l, send_l, recv_l)
    for third in range(3):
        project(third, 512, s_r2)
        send_part(third, s_r, d_r, send_r, recv_r)

    fetch[2].wait()
    part = dot(twice, w_out[...], 1, 0)
    w_last[:, 0:128] = jnp.where(even, part, 0.0).astype(BF16)
    w_last[:, 128:256] = jnp.where(even, 0.0, part).astype(BF16)
    half_gate = w_in[:, 512:640] * 0.5
    nothing = jnp.zeros((128, 128), BF16)
    w_gate[0:128, 0:128] = half_gate.astype(BF16)
    w_gate[0:128, 128:256] = nothing
    w_gate[128:256, 0:128] = nothing
    w_gate[128:256, 128:256] = half_gate.astype(BF16)

    def gate_body(third):
        def body(q, carry):
            out = dot(normed[third * 12 + q], w_gate[...], 1, 0)
            parts = []
            for b in range(4):
                j_row = x * 96 + third * 32 + lax.broadcasted_iota(jnp.int32, (32, 256), 0)
                i_lane = gx * 24 + 2 * q + lax.broadcasted_iota(jnp.int32, (32, 256), 1) // 128
                live = (j_row < my_len[b]) & (i_lane < my_len[b])
                half = out[b * 32 : (b + 1) * 32]
                parts.append(jnp.where(live, jnp.tanh(half) * 0.5 + 0.5, 0.0))
            gates[third * 12 + q] = jnp.concatenate(parts, axis=0)
            return carry

        steps(12, U_GATE, body, 0)

    for third in range(3):
        gate_body(third)

    for third in range(3):
        wait_part(recv_l.at[third])

        def turn(n, carry):
            c = n // 4
            col = lax.rem(n, 4)
            block = d_l2[c * 12 + third * 4 + col]
            turned[n, third * 128 : (third + 1) * 128, :] = block.T
            return carry

        lax.fori_loop(0, 8, turn, 0)

    lane4 = lax.broadcasted_iota(jnp.int32, (32, 512), 1) % 128 // 32

    def multiply(third, after):
        def body(r, carry):
            shift = lax.rem(r + 2 * core, 4)
            block = lax.rem(z + shift, 4)
            for c in range(2):
                right = jnp.concatenate(
                    [d_r2[c * 12 + third * 4 + col] for col in range(4)], axis=1
                )
                out = dot(turned[c * 4 + block], right, 1, 0)
                rows = []
                for t in range(3):
                    g = [out[t * 128 + b * 32 : t * 128 + (b + 1) * 32] for b in range(4)]
                    rows.append(
                        jnp.where(
                            lane4 == 0,
                            g[0],
                            jnp.where(lane4 == 1, g[1], jnp.where(lane4 == 2, g[2], g[3])),
                        )
                    )
                full = jnp.concatenate(rows, axis=0)
                for piece in range(4):
                    for col in range(4):
                        s_t[third, block * 4 + piece, col, :, c] = (
                            full[piece * 24 : (piece + 1) * 24, col * 128 : (col + 1) * 128]
                            .astype(BF16)
                            .reshape(12, 2, 128)
                        )

            after(block, jnp.where(shift == 0, 1, 0))
            return carry

        lax.fori_loop(1, 5, body, 0)
        d_t[third, :, pl.ds(me * 2, 2)] = s_t[third, gx, x]

    def send_back(third, oz, oy, ox, first, count, sem):
        pltpu.make_async_remote_copy(
            src_ref=s_t.at[third, oz * 4 + oy, ox, pl.ds(first, count)],
            dst_ref=d_t.at[third, pl.ds(first, count), pl.ds(me * 2, 2)],
            send_sem=send_t,
            recv_sem=sem,
            device_id=(core, oz, oy, ox),
            device_id_type=MESH_ID,
        ).start()

    def send_block(third, block, own, first, count, sem):
        def body(n, carry):
            for dx in range(4):
                send_back(third, block, lax.rem(y + n + dx, 4), xs[dx], first, count, sem)
            return carry

        lax.fori_loop(1, 4, body, 0)
        for dx in range(1, 4):
            send_back(third, block, ys[dx], xs[dx], first, count, sem)

        @pl.when(own == 0)
        def _():
            send_back(third, block, y, x, first, count, sem)

    def send_third(third, first, count, sem):
        to_others(lambda oz, oy, ox: send_back(third, oz, oy, ox, first, count, sem))

    def finish(third, first, count, total):
        def body(q, total):
            v = d_t2[third * 12 + q].astype(F32).reshape(32, 8, 128)

            def over_channels(array):
                s = jnp.sum(array, axis=0)
                s = s + pltpu.roll(s, 4, 0)
                s = s + pltpu.roll(s, 2, 0)
                return s * (1.0 / 128)

            v = v - over_channels(v)[None]
            v = v * lax.rsqrt(over_channels(v * v) + EPS)[None]
            out = dot(v.reshape(256, 128).astype(BF16), w_last[...], 0, 0)
            change = out * gates[third * 12 + q]
            for parity in range(2):
                new = pair_rows(2 * q + parity, third).astype(F32)
                new = (new + change[:, parity * 128 : (parity + 1) * 128]).astype(BF16)
                for b in range(4):
                    updated[b, 2 * q + parity, third * 32 : (third + 1) * 32, :] = new[
                        b * 32 : (b + 1) * 32
                    ]
                total = total + jnp.sum(jnp.abs(new.astype(F32)).reshape(16, 8, 128), axis=0)
            return total

        return steps(count, U_LAST, lambda n, carry: body(first + n, carry), total)

    def hold(block, own):
        pass

    wait_part(recv_r.at[0])
    multiply(0, hold)
    wait_part(recv_r.at[1])
    send_third(0, 0, 12, recv_t.at[0])
    multiply(1, hold)
    wait_part(recv_r.at[2])
    send_third(1, 0, 12, recv_t.at[1])
    multiply(2, lambda block, own: send_block(2, block, own, 0, 6, recv_t.at[2]))
    send_third(2, 6, 6, recv_t.at[3])
    total = jnp.zeros((8, 128), F32)
    for third in range(2):
        wait_part(recv_t.at[third])
        total = finish(third, 0, 12, total)
    wait_part(recv_t.at[2], 6)
    total = finish(2, 0, 6, total)
    wait_part(recv_t.at[3], 6)
    total = finish(2, 6, 6, total)
    mine = jnp.sum(total, axis=0, keepdims=True)
    s_plane[...] = mine
    d_plane[y * 4 + x] = mine
    for _ in range(3):
        wait_part(send_l)
        wait_part(send_r)
        wait_part(send_t)

    for dy in range(4):
        for dx in range(4):
            if dy or dx:
                pltpu.make_async_remote_copy(
                    src_ref=s_plane,
                    dst_ref=d_plane.at[y * 4 + x],
                    send_sem=send_m,
                    recv_sem=recv_plane,
                    device_id=(core, z, ys[dy], xs[dx]),
                    device_id_type=MESH_ID,
                ).start()
    rest = d_plane.at[pl.ds(0, 15)]
    pltpu.make_async_copy(rest, rest, recv_plane).wait()
    plane = jnp.sum(d_plane[...], axis=0)
    s_all[...] = plane
    d_all[core * 4 + z] = plane
    pltpu.make_async_copy(rest, rest, send_m).wait()
    for dz in range(4):
        for other_core in (core, 1 - core):
            if dz or other_core is not core:
                pltpu.make_async_remote_copy(
                    src_ref=s_all,
                    dst_ref=d_all.at[core * 4 + z],
                    send_sem=send_m,
                    recv_sem=recv_all,
                    device_id=(other_core, zs[dz], y, x),
                    device_id_type=MESH_ID,
                ).start()
    rest = d_all.at[pl.ds(0, 7)]
    pltpu.make_async_copy(rest, rest, recv_all).wait()
    everyone = jnp.sum(d_all[...], axis=0)
    magnitude[...] = jnp.sum(everyone, axis=1, keepdims=True) * (1.0 / entries)
    pltpu.make_async_copy(rest, rest, send_m).wait()


def per_device(entries, pair_repr, seq_lengths, weight_in, weight_out):
    vmem = pl.BlockSpec(memory_space=pltpu.VMEM)
    hbm = pl.BlockSpec(memory_space=pl.ANY)
    dma = pltpu.SemaphoreType.DMA
    updated, magnitude = pl.pallas_call(
        lambda *refs: kernel(entries, *refs),
        out_shape=(
            pltpu.VMEM(pair_repr.shape, BF16),
            jax.ShapeDtypeStruct((1, 1), F32),
        ),
        in_specs=[pl.BlockSpec(memory_space=pltpu.SMEM), hbm, hbm, hbm],
        out_specs=(vmem, vmem),
        scratch_shapes=[
            pltpu.VMEM(pair_repr.shape, BF16),
            pltpu.VMEM(weight_in.shape, BF16),
            pltpu.VMEM(weight_out.shape, BF16),
            pltpu.VMEM((3, 12, 128, 2, 128), BF16),
            pltpu.VMEM((3, 12, 128, 2, 128), BF16),
            pltpu.VMEM((2, 3, 4, 192, 2, 128), BF16),
            pltpu.VMEM((2, 3, 4, 192, 2, 128), BF16),
            pltpu.VMEM((8, 384, 384), BF16),
            pltpu.VMEM((3, 16, 4, 12, 2, 2, 128), BF16),
            pltpu.VMEM((3, 12, 128, 2, 128), BF16),
            pltpu.VMEM((36, 128, 256), BF16),
            pltpu.VMEM((36, 128, 256), F32),
            pltpu.VMEM((1024, 256), BF16),
            pltpu.VMEM((256, 256), BF16),
            pltpu.VMEM((256, 256), BF16),
            pltpu.VMEM((1, 128), F32),
            pltpu.VMEM((16, 1, 128), F32),
            pltpu.VMEM((1, 128), F32),
            pltpu.VMEM((8, 1, 128), F32),
            dma,
            dma,
            dma,
            dma,
            dma((3,)),
            dma((3,)),
            dma((4,)),
            dma,
            dma,
            dma((5,)),
        ],
        compiler_params=pltpu.CompilerParams(
            collective_id=0, has_side_effects=True, vmem_limit_bytes=56 * 2**20
        ),
        name="triangle",
    )(seq_lengths, pair_repr, weight_in, weight_out)
    return updated, magnitude.reshape(())


def solution(mesh):
    finer = Mesh(mesh.devices.reshape(mesh.shape["gz"], 4, 4, mesh.shape["gy"]), AXES)
    entries = float(8 * 384 * 384 * 128)
    return jax.shard_map(
        lambda *args: per_device(entries, *args),
        mesh=finer,
        in_specs=(P("gz", GX, "gy", None), P(), P(), P()),
        out_specs=(P("gz", GX, "gy", None), P()),
        check_vma=False,
    )
```

```python
import jax
import jax.numpy as jnp
from jax import lax
from jax.experimental import pallas as pl
from jax.experimental.pallas import tpu as pltpu
from jax.sharding import Mesh
from jax.sharding import PartitionSpec as P

AXES = ("gz", "gx_0", "gx_1", "gy")
GX = ("gx_0", "gx_1")
MESH_ID = pl.DeviceIdType.MESH
F32 = jnp.float32
BF16 = jnp.bfloat16
EPS = 1e-05
U_NORM = 3
U_PROJ = 2
U_GATE = 2
U_LAST = 3


def steps(count, unroll, body, carry):
    def several(n, carry):
        for u in range(unroll):
            carry = body(n * unroll + u, carry)
        return carry

    return lax.fori_loop(0, count // unroll, several, carry)


def dot(a, b, ca, cb):
    return lax.dot_general(a, b, (((ca,), (cb,)), ((), ())), preferred_element_type=F32)


def kernel(
    entries,
    lens, pair_hbm, w_in_hbm, w_out_hbm,
    updated, magnitude,
    pair, w_in, w_out,
    s_l, s_r, d_l, d_r, turned, s_t, d_t, normed, gates, w_proj, w_gate, w_last,
    s_all, d_all,
    send_l, send_r, send_t, send_m, recv_l, recv_r, recv_t, recv_all,
    fetched, slab,
):
    core, z, y, x = (lax.axis_index(a) for a in AXES)
    gx = z * 4 + y
    me = gx * 4 + x

    barrier = pltpu.get_barrier_semaphore()
    zs = [lax.rem(z + n, 4) for n in range(4)]
    ys = [lax.rem(y + n, 4) for n in range(4)]
    xs = [lax.rem(x + n, 4) for n in range(4)]
    cores = [core, 1 - core]
    far_first = sorted(
        ((dc, dz, dy, dx) for dc in range(2) for dz in range(4) for dy in range(4) for dx in range(4)),
        key=lambda d: -sum(min(n, 4 - n) for n in d[1:]),
    )[:-2] + [(1, 0, 0, 0)]
    everyone_else = [(cores[dc], zs[dz], ys[dy], xs[dx]) for dc, dz, dy, dx in far_first]
    for device, step in zip(everyone_else, far_first):
        if step[0] == 0 or step == (1, 0, 0, 0):
            pl.semaphore_signal(barrier, inc=1, device_id=device, device_id_type=MESH_ID)

    def columns(third):
        return pl.ds(third * 32, 32)

    fetch = [
        pltpu.make_async_copy(
            pair_hbm.at[:, :, columns(0)], pair.at[:, :, columns(0)], fetched.at[0]
        ),
        pltpu.make_async_copy(w_in_hbm, w_in, fetched.at[3]),
        pltpu.make_async_copy(w_out_hbm, w_out, fetched.at[4]),
        pltpu.make_async_copy(
            pair_hbm.at[:, :, columns(1)], pair.at[:, :, columns(1)], fetched.at[1]
        ),
        pltpu.make_async_copy(
            pair_hbm.at[:, :, columns(2)], pair.at[:, :, columns(2)], fetched.at[2]
        ),
    ]
    for copy in fetch:
        copy.start()

    row2 = lax.broadcasted_iota(jnp.int32, (256, 128), 0)
    col2 = lax.broadcasted_iota(jnp.int32, (256, 128), 1)
    twice = (row2 // 2 == col2).astype(BF16)
    even = row2 % 2 == 0
    def prepare():
        fetch[1].wait()
        for kind in range(4):
            part = dot(twice, w_in[:, kind * 128 : (kind + 1) * 128], 1, 1)
            part = part * (0.5 if kind % 2 else 1.0)
            rows = pl.ds(kind * 256, 256)
            w_proj[rows, 0:128] = jnp.where(even, part, 0.0).astype(BF16)
            w_proj[rows, 128:256] = jnp.where(even, 0.0, part).astype(BF16)

    my_len = [lens[core * 4 + b] for b in range(4)]
    lane = lax.broadcasted_iota(jnp.int32, (8, 128), 1)
    sub = lax.broadcasted_iota(jnp.int32, (8, 128), 0)
    group = lane // 32
    len_lane = jnp.where(
        group == 0,
        my_len[0],
        jnp.where(group == 1, my_len[1], jnp.where(group == 2, my_len[2], my_len[3])),
    )
    s_l2 = s_l.reshape(36, 256, 128)
    s_r2 = s_r.reshape(36, 256, 128)
    d_l2 = d_l.reshape(24, 384, 128)
    d_r2 = d_r.reshape(24, 384, 128)
    d_t2 = d_t.reshape(36, 256, 128)

    def pair_rows(row, third):
        return jnp.concatenate(
            [pair[b, row, third * 32 : (third + 1) * 32, :] for b in range(4)], axis=0
        )

    def normalize(third, first, count):
        def body(n, carry):
            q = first + n
            halves = []
            for parity in range(2):
                v = pair_rows(2 * q + parity, third).astype(F32)
                mean_value = jnp.sum(v, axis=1, keepdims=True) * (1.0 / 128)
                v = v - mean_value
                variance = jnp.sum(v * v, axis=1, keepdims=True) * (1.0 / 128)
                halves.append((v * lax.rsqrt(variance + EPS)).astype(BF16))
            normed[third * 12 + q] = jnp.concatenate(halves, axis=1)
            return carry

        steps(count, U_NORM, body, 0)

    def project(third, first, count, row, store):
        def body(n, carry):
            q = first + n
            out = dot(w_proj[row : row + 512, :], normed[third * 12 + q], 1, 1)
            i_lane = x * 96 + third * 32 + lane % 32
            k_sub = gx * 24 + 2 * q + sub % 2
            half_mask = jnp.where((i_lane < len_lane) & (k_sub < len_lane), 0.5, 0.0)
            value = out[0:256].reshape(32, 8, 128) * half_mask[None]
            gate = jnp.tanh(out[256:512]).reshape(32, 8, 128) + 1.0
            store[third * 12 + q] = (value * gate).reshape(256, 128).astype(BF16)
            return carry

        steps(count, U_PROJ, body, 0)

    def to_others(send):
        def body(n, carry):
            oz = lax.rem(z + n, 4)
            oy = lax.rem(y + n // 4, 4)
            for dx in range(4):
                send(lax.rem(oz + dx, 4), lax.rem(oy + dx, 4), xs[dx])
            return carry

        lax.fori_loop(1, 16, body, 0)
        for dx in range(1, 4):
            send(zs[dx], ys[dx], xs[dx])

    def send_part(third, first, count, source, target, send_sem, recv_sem):
        def send(oz, oy, ox):
            channel = (oz * 16 + oy * 4 + ox) * 2
            for c in range(2):
                pltpu.make_async_remote_copy(
                    src_ref=source.at[third, pl.ds(first, count), channel + c],
                    dst_ref=target.at[c, third, x, pl.ds(gx * 12 + first, count)],
                    send_sem=send_sem,
                    recv_sem=recv_sem.at[third],
                    device_id=(core, oz, oy, ox),
                    device_id_type=MESH_ID,
                ).start()

        to_others(send)
        for c in range(2):
            target[c, third, x, pl.ds(gx * 12 + first, count)] = source[
                third, first : first + count, me * 2 + c
            ]

    def wait_part(sem, rows=12):
        part = d_t.at[0, pl.ds(0, rows), pl.ds(0, 126)]
        pltpu.make_async_copy(part, part, sem).wait()

    for third in range(3):
        fetch[(0, 3, 4)[third]].wait()
        for first, count in ((0, 6), (6, 6)) if third == 0 else ((0, 12),):
            normalize(third, first, count)
            if third == 0 and first == 0:
                prepare()
            project(third, first, count, 0, s_l2)
            if third == 0 and first == 0:
                pl.semaphore_wait(barrier, 64)
                pl.semaphore_signal(
                    slab, inc=1, device_id=(1 - core, z, y, x), device_id_type=MESH_ID
                )
            send_part(third, first, count, s_l, d_l, send_l, recv_l)
    for third in range(3):
        project(third, 0, 12, 512, s_r2)
        send_part(third, 0, 12, s_r, d_r, send_r, recv_r)

    fetch[2].wait()
    part = dot(twice, w_out[...], 1, 0)
    w_last[:, 0:128] = jnp.where(even, part, 0.0).astype(BF16)
    w_last[:, 128:256] = jnp.where(even, 0.0, part).astype(BF16)
    half_gate = w_in[:, 512:640] * 0.5
    nothing = jnp.zeros((128, 128), BF16)
    w_gate[0:128, 0:128] = half_gate.astype(BF16)
    w_gate[0:128, 128:256] = nothing
    w_gate[128:256, 0:128] = nothing
    w_gate[128:256, 128:256] = half_gate.astype(BF16)

    def gate_body(third):
        def body(q, carry):
            out = dot(normed[third * 12 + q], w_gate[...], 1, 0)
            parts = []
            for b in range(4):
                j_row = x * 96 + third * 32 + lax.broadcasted_iota(jnp.int32, (32, 256), 0)
                i_lane = gx * 24 + 2 * q + lax.broadcasted_iota(jnp.int32, (32, 256), 1) // 128
                live = (j_row < my_len[b]) & (i_lane < my_len[b])
                half = out[b * 32 : (b + 1) * 32]
                parts.append(jnp.where(live, jnp.tanh(half) * 0.5 + 0.5, 0.0))
            gates[third * 12 + q] = jnp.concatenate(parts, axis=0)
            return carry

        steps(12, U_GATE, body, 0)

    for third in range(3):
        gate_body(third)

    for third in range(3):
        wait_part(recv_l.at[third])

        def turn(n, carry):
            c = n // 4
            col = lax.rem(n, 4)
            block = d_l2[c * 12 + third * 4 + col]
            turned[n, third * 128 : (third + 1) * 128, :] = block.T
            return carry

        lax.fori_loop(0, 8, turn, 0)

    lane4 = lax.broadcasted_iota(jnp.int32, (32, 512), 1) % 128 // 32

    def multiply(third, after):
        def body(r, carry):
            shift = lax.rem(r + 2 * core, 4)
            block = lax.rem(z + shift, 4)
            for c in range(2):
                right = jnp.concatenate(
                    [d_r2[c * 12 + third * 4 + col] for col in range(4)], axis=1
                )
                out = dot(turned[c * 4 + block], right, 1, 0)
                rows = []
                for t in range(3):
                    g = [out[t * 128 + b * 32 : t * 128 + (b + 1) * 32] for b in range(4)]
                    rows.append(
                        jnp.where(
                            lane4 == 0,
                            g[0],
                            jnp.where(lane4 == 1, g[1], jnp.where(lane4 == 2, g[2], g[3])),
                        )
                    )
                full = jnp.concatenate(rows, axis=0)
                for piece in range(4):
                    for col in range(4):
                        s_t[third, block * 4 + piece, col, :, c] = (
                            full[piece * 24 : (piece + 1) * 24, col * 128 : (col + 1) * 128]
                            .astype(BF16)
                            .reshape(12, 2, 128)
                        )

            after(block, jnp.where(shift == 0, 1, 0))
            return carry

        lax.fori_loop(1, 5, body, 0)
        d_t[third, :, pl.ds(me * 2, 2)] = s_t[third, gx, x]

    def send_back(third, oz, oy, ox, first, count, sem):
        pltpu.make_async_remote_copy(
            src_ref=s_t.at[third, oz * 4 + oy, ox, pl.ds(first, count)],
            dst_ref=d_t.at[third, pl.ds(first, count), pl.ds(me * 2, 2)],
            send_sem=send_t,
            recv_sem=sem,
            device_id=(core, oz, oy, ox),
            device_id_type=MESH_ID,
        ).start()

    def send_block(third, block, own, first, count, sem):
        def body(n, carry):
            for dx in range(4):
                send_back(third, block, lax.rem(y + n + dx, 4), xs[dx], first, count, sem)
            return carry

        lax.fori_loop(1, 4, body, 0)
        for dx in range(1, 4):
            send_back(third, block, ys[dx], xs[dx], first, count, sem)

        @pl.when(own == 0)
        def _():
            send_back(third, block, y, x, first, count, sem)

    def send_third(third, first, count, sem):
        to_others(lambda oz, oy, ox: send_back(third, oz, oy, ox, first, count, sem))

    def finish(third, first, count, total):
        def body(q, total):
            v = d_t2[third * 12 + q].astype(F32).reshape(32, 8, 128)

            def over_channels(array):
                s = jnp.sum(array, axis=0)
                s = s + pltpu.roll(s, 4, 0)
                s = s + pltpu.roll(s, 2, 0)
                return s * (1.0 / 128)

            v = v - over_channels(v)[None]
            v = v * lax.rsqrt(over_channels(v * v) + EPS)[None]
            out = dot(v.reshape(256, 128).astype(BF16), w_last[...], 0, 0)
            change = out * gates[third * 12 + q]
            for parity in range(2):
                new = pair_rows(2 * q + parity, third).astype(F32)
                new = (new + change[:, parity * 128 : (parity + 1) * 128]).astype(BF16)
                for b in range(4):
                    updated[b, 2 * q + parity, third * 32 : (third + 1) * 32, :] = new[
                        b * 32 : (b + 1) * 32
                    ]
                total = total + jnp.sum(jnp.abs(new.astype(F32)).reshape(16, 8, 128), axis=0)
            return total

        return steps(count, 3 if count == 3 else U_LAST, lambda n, carry: body(first + n, carry), total)

    def hold(block, own):
        pass

    wait_part(recv_r.at[0])
    multiply(0, hold)
    wait_part(recv_r.at[1])
    multiply(1, hold)
    send_third(0, 0, 12, recv_t.at[0])
    wait_part(recv_r.at[2])
    send_third(1, 0, 12, recv_t.at[1])
    multiply(2, lambda block, own: send_block(2, block, own, 0, 6, recv_t.at[2]))
    send_third(2, 6, 6, recv_t.at[3])
    total = jnp.zeros((8, 128), F32)
    for third in range(2):
        wait_part(recv_t.at[third])
        total = finish(third, 0, 12, total)
    wait_part(recv_t.at[2], 6)
    total = finish(2, 0, 6, total)
    wait_part(recv_t.at[3], 6)
    total = finish(2, 6, 6, total)

    flat = core * 64 + me
    mine = jnp.sum(total, axis=0, keepdims=True)
    s_all[...] = mine
    d_all[flat] = mine
    for _ in range(3):
        wait_part(send_l)
        wait_part(send_r)
        wait_part(send_t)
    pl.semaphore_wait(slab, 1)
    for device in everyone_else:
        pltpu.make_async_remote_copy(
            src_ref=s_all,
            dst_ref=d_all.at[flat],
            send_sem=send_m,
            recv_sem=recv_all,
            device_id=device,
            device_id_type=MESH_ID,
        ).start()
    rest = d_all.at[pl.ds(0, 127)]
    pltpu.make_async_copy(rest, rest, recv_all).wait()
    everyone = jnp.sum(d_all.reshape(128, 128)[...], axis=0, keepdims=True)
    magnitude[...] = jnp.sum(everyone, axis=1, keepdims=True) * (1.0 / entries)
    pltpu.make_async_copy(rest, rest, send_m).wait()


def per_device(entries, pair_repr, seq_lengths, weight_in, weight_out):
    vmem = pl.BlockSpec(memory_space=pltpu.VMEM)
    hbm = pl.BlockSpec(memory_space=pl.ANY)
    dma = pltpu.SemaphoreType.DMA
    updated, magnitude = pl.pallas_call(
        lambda *refs: kernel(entries, *refs),
        out_shape=(
            pltpu.VMEM(pair_repr.shape, BF16),
            jax.ShapeDtypeStruct((1, 1), F32),
        ),
        in_specs=[pl.BlockSpec(memory_space=pltpu.SMEM), hbm, hbm, hbm],
        out_specs=(vmem, vmem),
        scratch_shapes=[
            pltpu.VMEM(pair_repr.shape, BF16),
            pltpu.VMEM(weight_in.shape, BF16),
            pltpu.VMEM(weight_out.shape, BF16),
            pltpu.VMEM((3, 12, 128, 2, 128), BF16),
            pltpu.VMEM((3, 12, 128, 2, 128), BF16),
            pltpu.VMEM((2, 3, 4, 192, 2, 128), BF16),
            pltpu.VMEM((2, 3, 4, 192, 2, 128), BF16),
            pltpu.VMEM((8, 384, 384), BF16),
            pltpu.VMEM((3, 16, 4, 12, 2, 2, 128), BF16),
            pltpu.VMEM((3, 12, 128, 2, 128), BF16),
            pltpu.VMEM((36, 128, 256), BF16),
            pltpu.VMEM((36, 128, 256), F32),
            pltpu.VMEM((1024, 256), BF16),
            pltpu.VMEM((256, 256), BF16),
            pltpu.VMEM((256, 256), BF16),
            pltpu.VMEM((1, 128), F32),
            pltpu.VMEM((128, 1, 128), F32),
            dma,
            dma,
            dma,
            dma,
            dma((3,)),
            dma((3,)),
            dma((5,)),
            dma,
            dma((5,)),
            pltpu.SemaphoreType.REGULAR,
        ],
        compiler_params=pltpu.CompilerParams(
            collective_id=0, has_side_effects=True, vmem_limit_bytes=56 * 2**20
        ),
        name="triangle",
    )(seq_lengths, pair_repr, weight_in, weight_out)
    return updated, magnitude.reshape(())


def solution(mesh):
    finer = Mesh(mesh.devices.reshape(mesh.shape["gz"], 4, 4, mesh.shape["gy"]), AXES)
    entries = float(8 * 384 * 384 * 128)
    return jax.shard_map(
        lambda *args: per_device(entries, *args),
        mesh=finer,
        in_specs=(P("gz", GX, "gy", None), P(), P(), P()),
        out_specs=(P("gz", GX, "gy", None), P()),
        check_vma=False,
    )
```

```python
import jax
import jax.numpy as jnp
from jax import lax
from jax.experimental import pallas as pl
from jax.experimental.pallas import tpu as pltpu
from jax.sharding import Mesh
from jax.sharding import PartitionSpec as P

AXES = ("gz", "gx_0", "gx_1", "gy")
GX = ("gx_0", "gx_1")
MESH_ID = pl.DeviceIdType.MESH
F32 = jnp.float32
BF16 = jnp.bfloat16
EPS = 1e-05
U_NORM = 3
U_PROJ = 2
U_GATE = 2
U_LAST = 6


def steps(count, unroll, body, carry):
    def several(n, carry):
        for u in range(unroll):
            carry = body(n * unroll + u, carry)
        return carry

    return lax.fori_loop(0, count // unroll, several, carry)


def dot(a, b, ca, cb):
    return lax.dot_general(a, b, (((ca,), (cb,)), ((), ())), preferred_element_type=F32)


def kernel(
    entries,
    lens_hbm, pair_hbm, w_in_hbm, w_out_hbm,
    updated, magnitude,
    lens, pair, w_in, w_out,
    s_l, s_r, d_l, d_r, turned, across, s_t, d_t, normed, gates, w_proj, w_gate, w_last,
    s_all, d_all,
    send_l, send_r, send_t, send_m, recv_l, recv_r, recv_t, recv_all,
    fetched, slab,
):
    core, z, y, x = (lax.axis_index(a) for a in AXES)
    gx = z * 4 + y
    me = gx * 4 + x

    barrier = pltpu.get_barrier_semaphore()
    zs = [lax.rem(z + n, 4) for n in range(4)]
    ys = [lax.rem(y + n, 4) for n in range(4)]
    xs = [lax.rem(x + n, 4) for n in range(4)]
    cores = [core, 1 - core]
    far_first = sorted(
        ((dc, dz, dy, dx) for dc in range(2) for dz in range(4) for dy in range(4) for dx in range(4)),
        key=lambda d: -sum(min(n, 4 - n) for n in d[1:]),
    )[:-2] + [(1, 0, 0, 0)]
    everyone_else = [(cores[dc], zs[dz], ys[dy], xs[dx]) for dc, dz, dy, dx in far_first]
    for device, step in zip(everyone_else, far_first):
        if step[0] == 0 or step == (1, 0, 0, 0):
            pl.semaphore_signal(barrier, inc=1, device_id=device, device_id_type=MESH_ID)

    def columns(third):
        return pl.ds(third * 32, 32)

    fetch = [
        pltpu.make_async_copy(
            pair_hbm.at[:, :, columns(0)], pair.at[:, :, columns(0)], fetched.at[0]
        ),
        pltpu.make_async_copy(w_in_hbm, w_in, fetched.at[3]),
        pltpu.make_async_copy(w_out_hbm, w_out, fetched.at[4]),
        pltpu.make_async_copy(
            pair_hbm.at[:, :, columns(1)], pair.at[:, :, columns(1)], fetched.at[1]
        ),
        pltpu.make_async_copy(
            pair_hbm.at[:, :, columns(2)], pair.at[:, :, columns(2)], fetched.at[2]
        ),
    ]
    fetch.append(pltpu.make_async_copy(lens_hbm, lens, fetched.at[5]))
    for copy in fetch:
        copy.start()

    row2 = lax.broadcasted_iota(jnp.int32, (256, 128), 0)
    col2 = lax.broadcasted_iota(jnp.int32, (256, 128), 1)
    twice = (row2 // 2 == col2).astype(BF16)
    even = row2 % 2 == 0
    def prepare():
        fetch[1].wait()
        for kind in range(4):
            part = dot(twice, w_in[:, kind * 128 : (kind + 1) * 128], 1, 1)
            part = part * (0.5 if kind % 2 else 1.0)
            rows = pl.ds(kind * 256, 256)
            w_proj[rows, 0:128] = jnp.where(even, part, 0.0).astype(BF16)
            w_proj[rows, 128:256] = jnp.where(even, 0.0, part).astype(BF16)

    fetch[5].wait()
    my_len = [lens[core * 4 + b] for b in range(4)]
    lane = lax.broadcasted_iota(jnp.int32, (8, 128), 1)
    sub = lax.broadcasted_iota(jnp.int32, (8, 128), 0)
    group = lane // 32
    len_lane = jnp.where(
        group == 0,
        my_len[0],
        jnp.where(group == 1, my_len[1], jnp.where(group == 2, my_len[2], my_len[3])),
    )
    d_l2 = d_l.reshape(24, 384, 128)
    d_r2 = d_r.reshape(24, 384, 128)

    def pair_rows(row, third):
        return jnp.concatenate(
            [pair[b, row, third * 32 : (third + 1) * 32, :] for b in range(4)], axis=0
        )

    def normalize(third, first, count):
        def body(n, carry):
            q = first + n
            halves = []
            for parity in range(2):
                v = pair_rows(2 * q + parity, third).astype(F32)
                mean_value = jnp.sum(v, axis=1, keepdims=True) * (1.0 / 128)
                v = v - mean_value
                variance = jnp.sum(v * v, axis=1, keepdims=True) * (1.0 / 128)
                halves.append((v * lax.rsqrt(variance + EPS)).astype(BF16))
            normed[third * 12 + q] = jnp.concatenate(halves, axis=1)
            return carry

        steps(count, U_NORM, body, 0)

    def project(third, first, count, row, store):
        def body(n, carry):
            q = first + n
            out = dot(w_proj[row : row + 512, :], normed[third * 12 + q], 1, 1)
            i_lane = x * 96 + third * 32 + lane % 32
            k_sub = gx * 24 + 2 * q + sub % 2
            half_mask = jnp.where((i_lane < len_lane) & (k_sub < len_lane), 0.5, 0.0)
            value = out[0:256].reshape(32, 8, 128) * half_mask[None]
            gate = jnp.tanh(out[256:512]).reshape(32, 8, 128) + 1.0
            store[third * 12 + q] = (
                (value * gate).reshape(256, 128).astype(BF16).reshape(128, 2, 128)
            )
            return carry

        steps(count, U_PROJ, body, 0)

    def to_others(send):
        def body(n, carry):
            oz = lax.rem(z + n, 4)
            oy = lax.rem(y + n // 4, 4)
            for dx in range(4):
                send(lax.rem(oz + dx, 4), lax.rem(oy + dx, 4), xs[dx])
            return carry

        lax.fori_loop(1, 16, body, 0)
        for dx in range(1, 4):
            send(zs[dx], ys[dx], xs[dx])

    def send_part(third, first, count, source, target, send_sem, recv_sem):
        def send(oz, oy, ox):
            channel = (oz * 16 + oy * 4 + ox) * 2
            for c in range(2):
                pltpu.make_async_remote_copy(
                    src_ref=source.at[
                        third * 12 + first : third * 12 + first + count, channel + c
                    ],
                    dst_ref=target.at[c, third, x, pl.ds(gx * 12 + first, count)],
                    send_sem=send_sem,
                    recv_sem=recv_sem.at[third],
                    device_id=(core, oz, oy, ox),
                    device_id_type=MESH_ID,
                ).start()

        to_others(send)
        for c in range(2):
            target[c, third, x, pl.ds(gx * 12 + first, count)] = source[
                third * 12 + first : third * 12 + first + count, me * 2 + c
            ]

    def wait_part(sem, rows=12):
        part = s_t.at[0, pl.ds(0, 63), :, pl.ds(0, rows)]
        pltpu.make_async_copy(part, part, sem).wait()

    for third in range(3):
        fetch[(0, 3, 4)[third]].wait()
        for first, count in ((0, 6), (6, 6)) if third == 0 else ((0, 12),):
            normalize(third, first, count)
            if third == 0 and first == 0:
                prepare()
            project(third, first, count, 0, s_l)
            if third == 0 and first == 0:
                pl.semaphore_wait(barrier, 64)
                pl.semaphore_signal(
                    slab, inc=1, device_id=(1 - core, z, y, x), device_id_type=MESH_ID
                )
            send_part(third, first, count, s_l, d_l, send_l, recv_l)
    for third in range(3):
        project(third, 0, 12, 512, s_r)
        send_part(third, 0, 12, s_r, d_r, send_r, recv_r)

    fetch[2].wait()
    part = dot(twice, w_out[...], 1, 0)
    w_last[:, 0:128] = jnp.where(even, part, 0.0).astype(BF16)
    w_last[:, 128:256] = jnp.where(even, 0.0, part).astype(BF16)
    half_gate = w_in[:, 512:640] * 0.5
    nothing = jnp.zeros((128, 128), BF16)
    w_gate[0:128, 0:128] = half_gate.astype(BF16)
    w_gate[0:128, 128:256] = nothing
    w_gate[128:256, 0:128] = nothing
    w_gate[128:256, 128:256] = half_gate.astype(BF16)

    def gate_body(third):
        def body(q, carry):
            out = dot(normed[third * 12 + q], w_gate[...], 1, 0)
            parts = []
            for b in range(4):
                j_row = x * 96 + third * 32 + lax.broadcasted_iota(jnp.int32, (32, 256), 0)
                i_lane = gx * 24 + 2 * q + lax.broadcasted_iota(jnp.int32, (32, 256), 1) // 128
                live = (j_row < my_len[b]) & (i_lane < my_len[b])
                half = out[b * 32 : (b + 1) * 32]
                parts.append(jnp.where(live, jnp.tanh(half) * 0.5 + 0.5, 0.0))
            gates[third * 12 + q] = jnp.concatenate(parts, axis=0)
            return carry

        steps(12, U_GATE, body, 0)

    for third in range(3):
        gate_body(third)

    for third in range(3):
        wait_part(recv_l.at[third])

        def turn(n, carry):
            c = n // 4
            col = lax.rem(n, 4)
            block = d_l2[c * 12 + third * 4 + col]
            turned[n, third * 128 : (third + 1) * 128, :] = block.T
            return carry

        lax.fori_loop(0, 8, turn, 0)

    lane4 = lax.broadcasted_iota(jnp.int32, (32, 512), 1) % 128 // 32

    def multiply(third, after):
        for c in range(2):
            for col in range(4):
                across[c, :, col * 128 : (col + 1) * 128] = d_r2[c * 12 + third * 4 + col]

        def body(r, carry):
            shift = lax.rem(r + 2 * core, 4)
            block = lax.rem(z + shift, 4)
            for c in range(2):
                out = dot(turned[c * 4 + block], across[c], 1, 0)
                rows = []
                for t in range(3):
                    g = [out[t * 128 + b * 32 : t * 128 + (b + 1) * 32] for b in range(4)]
                    rows.append(
                        jnp.where(
                            lane4 == 0,
                            g[0],
                            jnp.where(lane4 == 1, g[1], jnp.where(lane4 == 2, g[2], g[3])),
                        )
                    )
                full = jnp.concatenate(rows, axis=0)
                for piece in range(4):
                    for col in range(4):
                        s_t[third, (block * 4 + piece) * 4 + col, c] = (
                            full[piece * 24 : (piece + 1) * 24, col * 128 : (col + 1) * 128]
                            .astype(BF16)
                            .reshape(12, 2, 128)
                        )

            after(block, jnp.where(shift == 0, 1, 0))
            return carry

        lax.fori_loop(1, 5, body, 0)
        whole = d_t.at[
            third * 12 : third * 12 + 12, pl.ds(pl.multiple_of(me // 2 * 8, 8), 8)
        ]
        for half in range(2):

            @pl.when(me % 2 == half)
            def _():
                for c in range(2):
                    whole[:, half * 4 + 2 * c : half * 4 + 2 * c + 2] = s_t[
                        third, gx * 4 + x, c
                    ]


    def send_back(third, oz, oy, ox, first, count, sem):
        for c in range(2):
            pltpu.make_async_remote_copy(
                src_ref=s_t.at[third, (oz * 4 + oy) * 4 + ox, c, first : first + count],
                dst_ref=d_t.at[
                    third * 12 + first : third * 12 + first + count,
                    pl.ds(pl.multiple_of(me * 4 + 2 * c, 2), 2),
                ],
                send_sem=send_t,
                recv_sem=sem,
                device_id=(core, oz, oy, ox),
                device_id_type=MESH_ID,
            ).start()

    def send_block(third, block, own, first, count, sem):
        def body(n, carry):
            for dx in range(4):
                send_back(third, block, lax.rem(y + n + dx, 4), xs[dx], first, count, sem)
            return carry

        lax.fori_loop(1, 4, body, 0)
        for dx in range(1, 4):
            send_back(third, block, ys[dx], xs[dx], first, count, sem)

        @pl.when(own == 0)
        def _():
            send_back(third, block, y, x, first, count, sem)

    def send_third(third, first, count, sem):
        to_others(lambda oz, oy, ox: send_back(third, oz, oy, ox, first, count, sem))

    def finish(third, first, count, total):
        def body(q, total):
            v = d_t[third * 12 + q].astype(F32)

            def over_channels(array):
                parts = [array[n * 8 : n * 8 + 8] for n in range(32)]
                while len(parts) > 1:
                    parts = [parts[n] + parts[n + 1] for n in range(0, len(parts), 2)]
                s = parts[0]
                s = s + pltpu.roll(s, 4, 0)
                s = s + pltpu.roll(s, 2, 0)
                return jnp.concatenate([s * (1.0 / 128)] * 32, axis=0)

            v = v - over_channels(v)
            v = v * lax.rsqrt(over_channels(v * v) + EPS)
            out = dot(v.astype(BF16), w_last[...], 0, 0)
            change = out * gates[third * 12 + q]
            for parity in range(2):
                new = pair_rows(2 * q + parity, third).astype(F32)
                new = (new + change[:, parity * 128 : (parity + 1) * 128]).astype(BF16)
                for b in range(4):
                    updated[b, 2 * q + parity, third * 32 : (third + 1) * 32, :] = new[
                        b * 32 : (b + 1) * 32
                    ]
                total = total + jnp.sum(jnp.abs(new.astype(F32)).reshape(16, 8, 128), axis=0)
            return total

        return steps(count, 3 if count == 3 else U_LAST, lambda n, carry: body(first + n, carry), total)

    def hold(block, own):
        pass

    wait_part(recv_r.at[0])
    multiply(0, hold)
    wait_part(recv_r.at[1])
    multiply(1, hold)
    send_third(0, 0, 12, recv_t.at[0])
    wait_part(recv_r.at[2])
    send_third(1, 0, 12, recv_t.at[1])
    multiply(2, lambda block, own: send_block(2, block, own, 0, 6, recv_t.at[2]))
    send_third(2, 6, 6, recv_t.at[3])
    total = jnp.zeros((8, 128), F32)
    for third in range(2):
        wait_part(recv_t.at[third])
        total = finish(third, 0, 12, total)
    wait_part(recv_t.at[2], 6)
    total = finish(2, 0, 6, total)
    wait_part(recv_t.at[3], 6)
    total = finish(2, 6, 6, total)

    flat = core * 64 + me
    mine = jnp.sum(total, axis=0, keepdims=True)
    s_all[...] = mine
    d_all[flat] = mine
    for _ in range(3):
        wait_part(send_l)
        wait_part(send_r)
        wait_part(send_t)
    pl.semaphore_wait(slab, 1)
    for device in everyone_else:
        pltpu.make_async_remote_copy(
            src_ref=s_all,
            dst_ref=d_all.at[flat],
            send_sem=send_m,
            recv_sem=recv_all,
            device_id=device,
            device_id_type=MESH_ID,
        ).start()
    rest = d_all.at[pl.ds(0, 127)]
    pltpu.make_async_copy(rest, rest, recv_all).wait()
    everyone = jnp.sum(d_all.reshape(128, 128)[...], axis=0, keepdims=True)
    magnitude[...] = jnp.sum(everyone, axis=1, keepdims=True) * (1.0 / entries)
    pltpu.make_async_copy(rest, rest, send_m).wait()


def per_device(entries, pair_repr, seq_lengths, weight_in, weight_out):
    vmem = pl.BlockSpec(memory_space=pltpu.VMEM)
    hbm = pl.BlockSpec(memory_space=pl.ANY)
    dma = pltpu.SemaphoreType.DMA
    updated, magnitude = pl.pallas_call(
        lambda *refs: kernel(entries, *refs),
        out_shape=(
            pltpu.VMEM(pair_repr.shape, BF16),
            pltpu.VMEM((1, 1), F32),
        ),
        in_specs=[hbm, hbm, hbm, hbm],
        out_specs=(vmem, vmem),
        scratch_shapes=[
            pltpu.SMEM(seq_lengths.shape, jnp.int32),
            pltpu.VMEM(pair_repr.shape, BF16),
            pltpu.VMEM(weight_in.shape, BF16),
            pltpu.VMEM(weight_out.shape, BF16),
            pltpu.VMEM((36, 128, 2, 128), BF16),
            pltpu.VMEM((36, 128, 2, 128), BF16),
            pltpu.VMEM((2, 3, 4, 192, 2, 128), BF16),
            pltpu.VMEM((2, 3, 4, 192, 2, 128), BF16),
            pltpu.VMEM((8, 384, 384), BF16),
            pltpu.VMEM((2, 384, 512), BF16),
            pltpu.VMEM((3, 64, 2, 12, 2, 128), BF16),
            pltpu.VMEM((36, 256, 128), BF16),
            pltpu.VMEM((36, 128, 256), BF16),
            pltpu.VMEM((36, 128, 256), F32),
            pltpu.VMEM((1024, 256), BF16),
            pltpu.VMEM((256, 256), BF16),
            pltpu.VMEM((256, 256), BF16),
            pltpu.VMEM((1, 128), F32),
            pltpu.VMEM((128, 1, 128), F32),
            dma,
            dma,
            dma,
            dma,
            dma((3,)),
            dma((3,)),
            dma((5,)),
            dma,
            dma((6,)),
            pltpu.SemaphoreType.REGULAR,
        ],
        compiler_params=pltpu.CompilerParams(
            collective_id=0, has_side_effects=True, vmem_limit_bytes=56 * 2**20
        ),
        name="triangle",
    )(seq_lengths, pair_repr, weight_in, weight_out)
    return updated, magnitude.reshape(())


def solution(mesh):
    finer = Mesh(mesh.devices.reshape(mesh.shape["gz"], 4, 4, mesh.shape["gy"]), AXES)
    entries = float(8 * 384 * 384 * 128)
    return jax.shard_map(
        lambda *args: per_device(entries, *args),
        mesh=finer,
        in_specs=(P("gz", GX, "gy", None), P(), P(), P()),
        out_specs=(P("gz", GX, "gy", None), P()),
        check_vma=False,
    )
```

```python
import jax
import jax.numpy as jnp
from jax import lax
from jax.experimental import pallas as pl
from jax.experimental.pallas import tpu as pltpu
from jax.sharding import Mesh
from jax.sharding import PartitionSpec as P

AXES = ("gz", "gx_0", "gx_1", "gy")
GX = ("gx_0", "gx_1")
MESH_ID = pl.DeviceIdType.MESH
F32 = jnp.float32
BF16 = jnp.bfloat16
EPS = 1e-05
U_NORM = 3
U_PROJ = 2
U_GATE = 2
U_LAST = 6


def steps(count, unroll, body, carry):
    def several(n, carry):
        for u in range(unroll):
            carry = body(n * unroll + u, carry)
        return carry

    return lax.fori_loop(0, count // unroll, several, carry)


def dot(a, b, ca, cb):
    return lax.dot_general(a, b, (((ca,), (cb,)), ((), ())), preferred_element_type=F32)


def kernel(
    lens_hbm, pair_hbm, w_in_hbm, w_out_hbm,
    updated, sums,
    lens, pair, w_in, w_out,
    s_l, s_r, d_l, d_r, turned, across, s_t, d_t, normed, gates, w_proj, w_gate, w_last,
    s_all, d_all,
    send_l, send_r, send_t, send_m, recv_l, recv_r, recv_t, recv_all,
    fetched, slab,
):
    core, z, y, x = (lax.axis_index(a) for a in AXES)
    gx = z * 4 + y
    me = gx * 4 + x

    def columns(third):
        return pl.ds(third * 32, 32)

    fetch = [
        pltpu.make_async_copy(
            pair_hbm.at[:, :, columns(0)], pair.at[:, :, columns(0)], fetched.at[0]
        ),
        pltpu.make_async_copy(w_in_hbm, w_in, fetched.at[3]),
        pltpu.make_async_copy(w_out_hbm, w_out, fetched.at[4]),
        pltpu.make_async_copy(
            pair_hbm.at[:, :, columns(1)], pair.at[:, :, columns(1)], fetched.at[1]
        ),
        pltpu.make_async_copy(
            pair_hbm.at[:, :, columns(2)], pair.at[:, :, columns(2)], fetched.at[2]
        ),
    ]
    fetch.append(pltpu.make_async_copy(lens_hbm, lens, fetched.at[5]))
    for copy in fetch:
        copy.start()

    barrier = pltpu.get_barrier_semaphore()
    zs = [lax.rem(z + n, 4) for n in range(4)]
    ys = [lax.rem(y + n, 4) for n in range(4)]
    xs = [lax.rem(x + n, 4) for n in range(4)]
    cores = [core, 1 - core]
    far_first = sorted(
        ((dc, dz, dy, dx) for dc in range(2) for dz in range(4) for dy in range(4) for dx in range(4)),
        key=lambda d: -sum(min(n, 4 - n) for n in d[1:]),
    )[:-2] + [(1, 0, 0, 0)]
    everyone_else = [(cores[dc], zs[dz], ys[dy], xs[dx]) for dc, dz, dy, dx in far_first]
    for device, step in zip(everyone_else, far_first):
        if step[0] == 0 or step == (1, 0, 0, 0):
            pl.semaphore_signal(barrier, inc=1, device_id=device, device_id_type=MESH_ID)


    row2 = lax.broadcasted_iota(jnp.int32, (256, 128), 0)
    col2 = lax.broadcasted_iota(jnp.int32, (256, 128), 1)
    twice = (row2 // 2 == col2).astype(BF16)
    even = row2 % 2 == 0
    def prepare():
        fetch[1].wait()
        for kind in range(4):
            part = dot(twice, w_in[:, kind * 128 : (kind + 1) * 128], 1, 1)
            part = part * (0.5 if kind % 2 else 1.0)
            rows = pl.ds(kind * 256, 256)
            w_proj[rows, 0:128] = jnp.where(even, part, 0.0).astype(BF16)
            w_proj[rows, 128:256] = jnp.where(even, 0.0, part).astype(BF16)

    fetch[5].wait()
    my_len = [lens[core * 4 + b] for b in range(4)]
    lane = lax.broadcasted_iota(jnp.int32, (8, 128), 1)
    sub = lax.broadcasted_iota(jnp.int32, (8, 128), 0)
    group = lane // 32
    len_lane = jnp.where(
        group == 0,
        my_len[0],
        jnp.where(group == 1, my_len[1], jnp.where(group == 2, my_len[2], my_len[3])),
    )
    d_l2 = d_l.reshape(24, 384, 128)
    d_r2 = d_r.reshape(24, 384, 128)

    def pair_rows(row, third):
        return jnp.concatenate(
            [pair[b, row, third * 32 : (third + 1) * 32, :] for b in range(4)], axis=0
        )

    def normalize(third, first, count):
        def body(n, carry):
            q = first + n
            halves = []
            for parity in range(2):
                v = pair_rows(2 * q + parity, third).astype(F32)
                mean_value = jnp.sum(v, axis=1, keepdims=True) * (1.0 / 128)
                v = v - mean_value
                variance = jnp.sum(v * v, axis=1, keepdims=True) * (1.0 / 128)
                halves.append((v * lax.rsqrt(variance + EPS)).astype(BF16))
            normed[third * 12 + q] = jnp.concatenate(halves, axis=1)
            return carry

        steps(count, U_NORM, body, 0)

    def project(third, first, count, row, store):
        def body(n, carry):
            q = first + n
            out = dot(w_proj[row : row + 512, :], normed[third * 12 + q], 1, 1)
            i_lane = x * 96 + third * 32 + lane % 32
            k_sub = gx * 24 + 2 * q + sub % 2
            half_mask = jnp.where((i_lane < len_lane) & (k_sub < len_lane), 0.5, 0.0)
            value = out[0:256].reshape(32, 8, 128) * half_mask[None]
            gate = jnp.tanh(out[256:512]).reshape(32, 8, 128) + 1.0
            store[third * 12 + q] = (
                (value * gate).reshape(256, 128).astype(BF16).reshape(128, 2, 128)
            )
            return carry

        steps(count, U_PROJ, body, 0)

    def to_others(send):
        sign = 1 + 2 * core
        mirrored = [lax.rem(x + dx * sign, 4) for dx in range(4)]

        def body(n, carry):
            oz = z + n * sign
            oy = y + n // 4 * sign
            for dx in range(4):
                send(lax.rem(oz + dx * sign, 4), lax.rem(oy + dx * sign, 4), mirrored[dx])
            return carry

        lax.fori_loop(1, 16, body, 0)
        for dx in range(1, 4):
            send(zs[dx], ys[dx], xs[dx])

    def send_part(third, first, count, source, target, send_sem, recv_sem):
        def send(oz, oy, ox):
            channel = (oz * 16 + oy * 4 + ox) * 2
            for c in range(2):
                pltpu.make_async_remote_copy(
                    src_ref=source.at[
                        third * 12 + first : third * 12 + first + count, channel + c
                    ],
                    dst_ref=target.at[c, third, x, pl.ds(gx * 12 + first, count)],
                    send_sem=send_sem,
                    recv_sem=recv_sem.at[third],
                    device_id=(core, oz, oy, ox),
                    device_id_type=MESH_ID,
                ).start()

        for c in range(2):
            target[c, third, x, pl.ds(gx * 12 + first, count)] = source[
                third * 12 + first : third * 12 + first + count, me * 2 + c
            ]

        to_others(send)

    def wait_part(sem, rows=12):
        part = s_t.at[0, pl.ds(0, 63), pl.ds(0, rows)]
        pltpu.make_async_copy(part, part, sem).wait()

    for third in range(3):
        fetch[(0, 3, 4)[third]].wait()
        for first, count in ((0, 6), (6, 6)) if third == 0 else ((0, 12),):
            normalize(third, first, count)
            if third == 0 and first == 0:
                prepare()
            project(third, first, count, 0, s_l)
            if third == 0 and first == 0:
                pl.semaphore_wait(barrier, 64)
                pl.semaphore_signal(
                    slab, inc=1, device_id=(1 - core, z, y, x), device_id_type=MESH_ID
                )
            send_part(third, first, count, s_l, d_l, send_l, recv_l)
    for third in range(3):
        project(third, 0, 12, 512, s_r)
        send_part(third, 0, 12, s_r, d_r, send_r, recv_r)

    fetch[2].wait()
    part = dot(twice, w_out[...], 1, 0)
    w_last[:, 0:128] = jnp.where(even, part, 0.0).astype(BF16)
    w_last[:, 128:256] = jnp.where(even, 0.0, part).astype(BF16)
    half_gate = w_in[:, 512:640] * 0.5
    nothing = jnp.zeros((128, 128), BF16)
    w_gate[0:128, 0:128] = half_gate.astype(BF16)
    w_gate[0:128, 128:256] = nothing
    w_gate[128:256, 0:128] = nothing
    w_gate[128:256, 128:256] = half_gate.astype(BF16)

    def gate_body(third):
        def body(q, carry):
            out = dot(normed[third * 12 + q], w_gate[...], 1, 0)
            parts = []
            for b in range(4):
                j_row = x * 96 + third * 32 + lax.broadcasted_iota(jnp.int32, (32, 256), 0)
                i_lane = gx * 24 + 2 * q + lax.broadcasted_iota(jnp.int32, (32, 256), 1) // 128
                live = (j_row < my_len[b]) & (i_lane < my_len[b])
                half = out[b * 32 : (b + 1) * 32]
                parts.append(jnp.where(live, jnp.tanh(half) * 0.5 + 0.5, 0.0))
            gates[third * 12 + q] = jnp.concatenate(parts, axis=0)
            return carry

        steps(12, U_GATE, body, 0)

    for third in range(3):
        gate_body(third)

    for third in range(3):
        wait_part(recv_l.at[third])

        def turn(n, carry):
            c = n // 4
            col = lax.rem(n, 4)
            block = d_l2[c * 12 + third * 4 + col]
            turned[n, third * 128 : (third + 1) * 128, :] = block.T
            return carry

        lax.fori_loop(0, 8, turn, 0)

    lane4 = lax.broadcasted_iota(jnp.int32, (32, 512), 1) % 128 // 32

    def multiply(third, after):
        def place(r):
            shift = lax.rem(r + 2 * core, 4)
            return lax.rem(z + shift, 4), jnp.where(shift == 0, 1, 0)

        def leave(r):
            after(*place(r))

        for c in range(2):
            for col in range(4):
                across[c, :, col * 128 : (col + 1) * 128] = d_r2[c * 12 + third * 4 + col]

        def body(r, carry):
            block = place(r)[0]
            full = []
            for c in range(2):
                out = dot(turned[c * 4 + block], across[c], 1, 0)
                rows = []
                for t in range(3):
                    g = [out[t * 128 + b * 32 : t * 128 + (b + 1) * 32] for b in range(4)]
                    rows.append(
                        jnp.where(
                            lane4 == 0,
                            g[0],
                            jnp.where(lane4 == 1, g[1], jnp.where(lane4 == 2, g[2], g[3])),
                        )
                    )
                full.append(jnp.concatenate(rows, axis=0))
            for piece in range(4):
                for col in range(4):
                    here = [
                        f[piece * 24 : (piece + 1) * 24, col * 128 : (col + 1) * 128]
                        .astype(BF16)
                        .reshape(12, 2, 128)
                        for f in full
                    ]
                    s_t[third, (block * 4 + piece) * 4 + col] = jnp.concatenate(here, axis=1)
            leave(r)
            return carry

        lax.fori_loop(1, 5, body, 0)
        whole = d_t.at[
            third * 12 : third * 12 + 12, pl.ds(pl.multiple_of(me // 2 * 8, 8), 8)
        ]
        for half in range(2):

            @pl.when(me % 2 == half)
            def _():
                whole[:, half * 4 : half * 4 + 4] = s_t[third, gx * 4 + x]


    def send_back(third, oz, oy, ox, first, count, sem):
        pltpu.make_async_remote_copy(
            src_ref=s_t.at[third, (oz * 4 + oy) * 4 + ox, first : first + count],
            dst_ref=d_t.at[
                third * 12 + first : third * 12 + first + count,
                pl.ds(pl.multiple_of(me * 4, 4), 4),
            ],
            send_sem=send_t,
            recv_sem=sem,
            device_id=(core, oz, oy, ox),
            device_id_type=MESH_ID,
        ).start()

    def send_block(third, block, own, first, count, sem):
        def body(n, carry):
            for dx in range(4):
                send_back(third, block, lax.rem(y + n + dx, 4), xs[dx], first, count, sem)
            return carry

        lax.fori_loop(1, 4, body, 0)
        for dx in range(1, 4):
            send_back(third, block, ys[dx], xs[dx], first, count, sem)

        @pl.when(own == 0)
        def _():
            send_back(third, block, y, x, first, count, sem)

    def send_third(third, first, count, sem):
        to_others(lambda oz, oy, ox: send_back(third, oz, oy, ox, first, count, sem))

    def finish(third, first, count, total):
        def body(q, total):
            v = d_t[third * 12 + q].astype(F32)

            def over_channels(array):
                parts = [array[n * 8 : n * 8 + 8] for n in range(32)]
                while len(parts) > 1:
                    parts = [parts[n] + parts[n + 1] for n in range(0, len(parts), 2)]
                s = parts[0]
                s = s + pltpu.roll(s, 4, 0)
                s = s + pltpu.roll(s, 2, 0)
                return jnp.concatenate([s * (1.0 / 128)] * 32, axis=0)

            v = v - over_channels(v)
            v = v * lax.rsqrt(over_channels(v * v) + EPS)
            out = dot(v.astype(BF16), w_last[...], 0, 0)
            change = out * gates[third * 12 + q]
            for parity in range(2):
                new = pair_rows(2 * q + parity, third).astype(F32)
                new = (new + change[:, parity * 128 : (parity + 1) * 128]).astype(BF16)
                for b in range(4):
                    updated[b, 2 * q + parity, third * 32 : (third + 1) * 32, :] = new[
                        b * 32 : (b + 1) * 32
                    ]
                total = total + jnp.sum(jnp.abs(new.astype(F32)).reshape(16, 8, 128), axis=0)
            return total

        return steps(count, 3 if count == 3 else U_LAST, lambda n, carry: body(first + n, carry), total)

    def hold(block, own):
        pass

    wait_part(recv_r.at[0])
    multiply(0, hold)
    wait_part(recv_r.at[1])
    send_third(0, 0, 12, recv_t.at[0])
    multiply(1, hold)
    wait_part(recv_r.at[2])
    send_third(1, 0, 12, recv_t.at[1])
    multiply(2, lambda block, own: send_block(2, block, own, 0, 6, recv_t.at[2]))
    send_third(2, 6, 6, recv_t.at[3])
    total = jnp.zeros((8, 128), F32)
    for third in range(2):
        wait_part(recv_t.at[third])
        total = finish(third, 0, 12, total)
    wait_part(recv_t.at[2], 6)
    total = finish(2, 0, 6, total)
    wait_part(recv_t.at[3], 6)
    total = finish(2, 6, 6, total)

    flat = core * 64 + me
    mine = jnp.sum(total, axis=0, keepdims=True)
    s_all[...] = mine
    d_all[flat] = mine
    for _ in range(3):
        wait_part(send_l)
        wait_part(send_r)
        wait_part(send_t)
    pl.semaphore_wait(slab, 1)
    for device in everyone_else:
        pltpu.make_async_remote_copy(
            src_ref=s_all,
            dst_ref=d_all.at[flat],
            send_sem=send_m,
            recv_sem=recv_all,
            device_id=device,
            device_id_type=MESH_ID,
        ).start()
    rest = d_all.at[pl.ds(0, 127)]
    pltpu.make_async_copy(rest, rest, recv_all).wait()
    sums[...] = jnp.sum(d_all.reshape(128, 128)[...].reshape(16, 8, 128), axis=0)
    pltpu.make_async_copy(rest, rest, send_m).wait()


def hand_over(entries, updated, sums, out, total, done):
    copies = [pltpu.make_async_copy(updated.at[b], out.at[b], done.at[b]) for b in range(4)]
    for copy in copies:
        copy.start()
    everyone = jnp.sum(sums[...], axis=0, keepdims=True)
    total[...] = jnp.sum(everyone, axis=1, keepdims=True) * (1.0 / entries)
    for copy in copies:
        copy.wait()


def per_device(entries, pair_repr, seq_lengths, weight_in, weight_out):
    vmem = pl.BlockSpec(memory_space=pltpu.VMEM)
    hbm = pl.BlockSpec(memory_space=pl.ANY)
    dma = pltpu.SemaphoreType.DMA
    updated, sums = pl.pallas_call(
        kernel,
        out_shape=(
            pltpu.VMEM(pair_repr.shape, BF16),
            pltpu.VMEM((8, 128), F32),
        ),
        in_specs=[hbm, hbm, hbm, hbm],
        out_specs=(vmem, vmem),
        scratch_shapes=[
            pltpu.SMEM(seq_lengths.shape, jnp.int32),
            pltpu.VMEM(pair_repr.shape, BF16),
            pltpu.VMEM(weight_in.shape, BF16),
            pltpu.VMEM(weight_out.shape, BF16),
            pltpu.VMEM((36, 128, 2, 128), BF16),
            pltpu.VMEM((36, 128, 2, 128), BF16),
            pltpu.VMEM((2, 3, 4, 192, 2, 128), BF16),
            pltpu.VMEM((2, 3, 4, 192, 2, 128), BF16),
            pltpu.VMEM((8, 384, 384), BF16),
            pltpu.VMEM((2, 384, 512), BF16),
            pltpu.VMEM((3, 64, 12, 4, 128), BF16),
            pltpu.VMEM((36, 256, 128), BF16),
            pltpu.VMEM((36, 128, 256), BF16),
            pltpu.VMEM((36, 128, 256), F32),
            pltpu.VMEM((1024, 256), BF16),
            pltpu.VMEM((256, 256), BF16),
            pltpu.VMEM((256, 256), BF16),
            pltpu.VMEM((1, 128), F32),
            pltpu.VMEM((128, 1, 128), F32),
            dma,
            dma,
            dma,
            dma,
            dma((3,)),
            dma((3,)),
            dma((5,)),
            dma,
            dma((6,)),
            pltpu.SemaphoreType.REGULAR,
        ],
        compiler_params=pltpu.CompilerParams(
            collective_id=0, has_side_effects=True, vmem_limit_bytes=56 * 2**20
        ),
        name="triangle",
    )(seq_lengths, pair_repr, weight_in, weight_out)
    out, total = pl.pallas_call(
        lambda *refs: hand_over(entries, *refs),
        out_shape=(
            jax.ShapeDtypeStruct(pair_repr.shape, BF16),
            jax.ShapeDtypeStruct((1, 1), F32),
        ),
        in_specs=[vmem, vmem],
        out_specs=(hbm, vmem),
        scratch_shapes=[dma((4,))],
        compiler_params=pltpu.CompilerParams(vmem_limit_bytes=2**20),
        name="hand_over",
    )(updated, sums)
    return out, total.reshape(())


def solution(mesh):
    finer = Mesh(mesh.devices.reshape(mesh.shape["gz"], 4, 4, mesh.shape["gy"]), AXES)
    entries = float(8 * 384 * 384 * 128)
    return jax.shard_map(
        lambda *args: per_device(entries, *args),
        mesh=finer,
        in_specs=(P("gz", GX, "gy", None), P(), P(), P()),
        out_specs=(P("gz", GX, "gy", None), P()),
        check_vma=False,
    )
```

```python
import jax
import jax.numpy as jnp
from jax import lax
from jax.experimental import pallas as pl
from jax.experimental.pallas import tpu as pltpu
from jax.sharding import Mesh
from jax.sharding import PartitionSpec as P

AXES = ("gz", "gx_0", "gx_1", "gy")
GX = ("gx_0", "gx_1")
MESH_ID = pl.DeviceIdType.MESH
F32 = jnp.float32
BF16 = jnp.bfloat16
EPS = 1e-05
U_NORM = 3
U_PROJ = 2
U_GATE = 2
U_LAST = 6


def steps(count, unroll, body, carry):
    def several(n, carry):
        for u in range(unroll):
            carry = body(n * unroll + u, carry)
        return carry

    return lax.fori_loop(0, count // unroll, several, carry)


def dot(a, b, ca, cb):
    return lax.dot_general(a, b, (((ca,), (cb,)), ((), ())), preferred_element_type=F32)


def kernel(
    lens_hbm, pair_hbm, w_in_hbm, w_out_hbm,
    updated, sums,
    lens, pair, w_in, w_out,
    s_l, s_r, d_l, d_r, turned, across, s_t, d_t, normed, gates, w_proj, w_gate, w_last,
    s_all, d_all,
    send_l, send_r, send_t, send_m, recv_l, recv_r, recv_t, recv_all,
    fetched, slab,
):
    core, z, y, x = (lax.axis_index(a) for a in AXES)
    gx = z * 4 + y
    me = gx * 4 + x

    def columns(third):
        return pl.ds(third * 32, 32)

    fetch = [
        pltpu.make_async_copy(
            pair_hbm.at[:, :, columns(0)], pair.at[:, :, columns(0)], fetched.at[0]
        ),
        pltpu.make_async_copy(w_in_hbm, w_in, fetched.at[3]),
        pltpu.make_async_copy(w_out_hbm, w_out, fetched.at[4]),
        pltpu.make_async_copy(
            pair_hbm.at[:, :, columns(1)], pair.at[:, :, columns(1)], fetched.at[1]
        ),
        pltpu.make_async_copy(
            pair_hbm.at[:, :, columns(2)], pair.at[:, :, columns(2)], fetched.at[2]
        ),
    ]
    fetch.append(pltpu.make_async_copy(lens_hbm, lens, fetched.at[5]))
    for copy in fetch:
        copy.start()

    barrier = pltpu.get_barrier_semaphore()
    zs = [lax.rem(z + n, 4) for n in range(4)]
    ys = [lax.rem(y + n, 4) for n in range(4)]
    xs = [lax.rem(x + n, 4) for n in range(4)]
    cores = [core, 1 - core]
    far_first = sorted(
        ((dc, dz, dy, dx) for dc in range(2) for dz in range(4) for dy in range(4) for dx in range(4)),
        key=lambda d: -sum(min(n, 4 - n) for n in d[1:]),
    )[:-2] + [(1, 0, 0, 0)]
    everyone_else = [(cores[dc], zs[dz], ys[dy], xs[dx]) for dc, dz, dy, dx in far_first]
    for device, step in zip(everyone_else, far_first):
        if step[0] == 0 or step == (1, 0, 0, 0):
            pl.semaphore_signal(barrier, inc=1, device_id=device, device_id_type=MESH_ID)


    row2 = lax.broadcasted_iota(jnp.int32, (256, 128), 0)
    col2 = lax.broadcasted_iota(jnp.int32, (256, 128), 1)
    twice = (row2 // 2 == col2).astype(BF16)
    even = row2 % 2 == 0
    def prepare():
        fetch[1].wait()
        for kind in range(4):
            part = dot(twice, w_in[:, kind * 128 : (kind + 1) * 128], 1, 1)
            part = part * (0.5 if kind % 2 else 1.0)
            rows = pl.ds(kind * 256, 256)
            w_proj[rows, 0:128] = jnp.where(even, part, 0.0).astype(BF16)
            w_proj[rows, 128:256] = jnp.where(even, 0.0, part).astype(BF16)

    fetch[5].wait()
    my_len = [lens[core * 4 + b] for b in range(4)]
    lane = lax.broadcasted_iota(jnp.int32, (8, 128), 1)
    sub = lax.broadcasted_iota(jnp.int32, (8, 128), 0)
    group = lane // 32
    len_lane = jnp.where(
        group == 0,
        my_len[0],
        jnp.where(group == 1, my_len[1], jnp.where(group == 2, my_len[2], my_len[3])),
    )
    d_l2 = d_l.reshape(24, 384, 128)
    d_r2 = d_r.reshape(24, 384, 128)

    def pair_rows(row, third):
        return jnp.concatenate(
            [pair[b, row, third * 32 : (third + 1) * 32, :] for b in range(4)], axis=0
        )

    def normalize(third, first, count):
        def body(n, carry):
            q = first + n
            halves = []
            for parity in range(2):
                v = pair_rows(2 * q + parity, third).astype(F32)
                mean_value = jnp.sum(v, axis=1, keepdims=True) * (1.0 / 128)
                v = v - mean_value
                variance = jnp.sum(v * v, axis=1, keepdims=True) * (1.0 / 128)
                halves.append((v * lax.rsqrt(variance + EPS)).astype(BF16))
            normed[third * 12 + q] = jnp.concatenate(halves, axis=1)
            return carry

        steps(count, U_NORM, body, 0)

    def project(third, first, count, row, store):
        def body(n, carry):
            q = first + n
            out = dot(w_proj[row : row + 512, :], normed[third * 12 + q], 1, 1)
            i_lane = x * 96 + third * 32 + lane % 32
            k_sub = gx * 24 + 2 * q + sub % 2
            half_mask = jnp.where((i_lane < len_lane) & (k_sub < len_lane), 0.5, 0.0)
            value = out[0:256].reshape(32, 8, 128) * half_mask[None]
            gate = jnp.tanh(out[256:512]).reshape(32, 8, 128) + 1.0
            store[third * 12 + q] = (
                (value * gate).reshape(256, 128).astype(BF16).reshape(128, 2, 128)
            )
            return carry

        steps(count, U_PROJ, body, 0)

    def to_others(send):
        sign = 1 + 2 * core
        mirrored = [lax.rem(x + dx * sign, 4) for dx in range(4)]

        def body(n, carry):
            oz = z + n * sign
            oy = y + n // 4 * sign
            for dx in range(4):
                send(lax.rem(oz + dx * sign, 4), lax.rem(oy + dx * sign, 4), mirrored[dx])
            return carry

        lax.fori_loop(1, 16, body, 0)
        for dx in range(1, 4):
            send(zs[dx], ys[dx], xs[dx])

    def send_part(third, first, count, source, target, send_sem, recv_sem):
        def send(oz, oy, ox):
            channel = (oz * 16 + oy * 4 + ox) * 2
            for c in range(2):
                pltpu.make_async_remote_copy(
                    src_ref=source.at[
                        third * 12 + first : third * 12 + first + count, channel + c
                    ],
                    dst_ref=target.at[c, third, x, pl.ds(gx * 12 + first, count)],
                    send_sem=send_sem,
                    recv_sem=recv_sem.at[third],
                    device_id=(core, oz, oy, ox),
                    device_id_type=MESH_ID,
                ).start()

        for c in range(2):
            target[c, third, x, pl.ds(gx * 12 + first, count)] = source[
                third * 12 + first : third * 12 + first + count, me * 2 + c
            ]

        to_others(send)

    def wait_part(sem, rows=12):
        part = s_t.at[0, pl.ds(0, 63), pl.ds(0, rows)]
        pltpu.make_async_copy(part, part, sem).wait()

    for third in range(3):
        fetch[(0, 3, 4)[third]].wait()
        for first, count in ((0, 6), (6, 6)) if third == 0 else ((0, 12),):
            normalize(third, first, count)
            if third == 0 and first == 0:
                prepare()
            project(third, first, count, 0, s_l)
            if third == 0 and first == 0:
                pl.semaphore_wait(barrier, 64)
                pl.semaphore_signal(
                    slab, inc=1, device_id=(1 - core, z, y, x), device_id_type=MESH_ID
                )
            send_part(third, first, count, s_l, d_l, send_l, recv_l)
    for third in range(3):
        project(third, 0, 12, 512, s_r)
        send_part(third, 0, 12, s_r, d_r, send_r, recv_r)

    fetch[2].wait()
    part = dot(twice, w_out[...], 1, 0)
    w_last[:, 0:128] = jnp.where(even, part, 0.0).astype(BF16)
    w_last[:, 128:256] = jnp.where(even, 0.0, part).astype(BF16)
    half_gate = w_in[:, 512:640] * 0.5
    nothing = jnp.zeros((128, 128), BF16)
    w_gate[0:128, 0:128] = half_gate.astype(BF16)
    w_gate[0:128, 128:256] = nothing
    w_gate[128:256, 0:128] = nothing
    w_gate[128:256, 128:256] = half_gate.astype(BF16)

    def gate_body(third):
        def body(q, carry):
            out = dot(normed[third * 12 + q], w_gate[...], 1, 0)
            parts = []
            for b in range(4):
                j_row = x * 96 + third * 32 + lax.broadcasted_iota(jnp.int32, (32, 256), 0)
                i_lane = gx * 24 + 2 * q + lax.broadcasted_iota(jnp.int32, (32, 256), 1) // 128
                live = (j_row < my_len[b]) & (i_lane < my_len[b])
                half = out[b * 32 : (b + 1) * 32]
                parts.append(jnp.where(live, jnp.tanh(half) * 0.5 + 0.5, 0.0))
            gates[third * 12 + q] = jnp.concatenate(parts, axis=0)
            return carry

        steps(12, U_GATE, body, 0)

    for third in range(3):
        gate_body(third)

    for third in range(3):
        wait_part(recv_l.at[third])

        def turn(n, carry):
            c = n // 4
            col = lax.rem(n, 4)
            block = d_l2[c * 12 + third * 4 + col]
            turned[n, third * 128 : (third + 1) * 128, :] = block.T
            return carry

        lax.fori_loop(0, 8, turn, 0)

    lane4 = lax.broadcasted_iota(jnp.int32, (32, 512), 1) % 128 // 32

    def multiply(third, after):
        def place(r):
            shift = lax.rem(r + 2 * core, 4)
            return lax.rem(z + shift, 4), jnp.where(shift == 0, 1, 0)

        def leave(r):
            after(*place(r))

        for c in range(2):
            for col in range(4):
                across[c, :, col * 128 : (col + 1) * 128] = d_r2[c * 12 + third * 4 + col]

        def body(r, carry):
            block = place(r)[0]
            full = []
            for c in range(2):
                out = dot(turned[c * 4 + block], across[c], 1, 0)
                rows = []
                for t in range(3):
                    g = [out[t * 128 + b * 32 : t * 128 + (b + 1) * 32] for b in range(4)]
                    rows.append(
                        jnp.where(
                            lane4 == 0,
                            g[0],
                            jnp.where(lane4 == 1, g[1], jnp.where(lane4 == 2, g[2], g[3])),
                        )
                    )
                full.append(jnp.concatenate(rows, axis=0))
            for piece in range(4):
                for col in range(4):
                    here = [
                        f[piece * 24 : (piece + 1) * 24, col * 128 : (col + 1) * 128]
                        .astype(BF16)
                        .reshape(12, 2, 128)
                        for f in full
                    ]
                    s_t[third, (block * 4 + piece) * 4 + col] = jnp.concatenate(here, axis=1)
            leave(r)
            return carry

        lax.fori_loop(1, 5, body, 0)
        whole = d_t.at[
            third * 12 : third * 12 + 12, pl.ds(pl.multiple_of(me // 2 * 8, 8), 8)
        ]
        for half in range(2):

            @pl.when(me % 2 == half)
            def _():
                whole[:, half * 4 : half * 4 + 4] = s_t[third, gx * 4 + x]


    def send_back(third, oz, oy, ox, first, count, sem):
        pltpu.make_async_remote_copy(
            src_ref=s_t.at[third, (oz * 4 + oy) * 4 + ox, first : first + count],
            dst_ref=d_t.at[
                third * 12 + first : third * 12 + first + count,
                pl.ds(pl.multiple_of(me * 4, 4), 4),
            ],
            send_sem=send_t,
            recv_sem=sem,
            device_id=(core, oz, oy, ox),
            device_id_type=MESH_ID,
        ).start()

    def send_block(third, block, own, first, count, sem):
        def body(n, carry):
            for dx in range(4):
                send_back(third, block, lax.rem(y + n + dx, 4), xs[dx], first, count, sem)
            return carry

        lax.fori_loop(1, 4, body, 0)
        for dx in range(1, 4):
            send_back(third, block, ys[dx], xs[dx], first, count, sem)

        @pl.when(own == 0)
        def _():
            send_back(third, block, y, x, first, count, sem)

    def send_third(third, first, count, sem):
        to_others(lambda oz, oy, ox: send_back(third, oz, oy, ox, first, count, sem))

    def finish(third, first, count, total):
        def body(q, total):
            v = d_t[third * 12 + q].astype(F32)

            def over_channels(array):
                parts = [array[n * 8 : n * 8 + 8] for n in range(32)]
                while len(parts) > 1:
                    parts = [parts[n] + parts[n + 1] for n in range(0, len(parts), 2)]
                s = parts[0]
                s = s + pltpu.roll(s, 4, 0)
                s = s + pltpu.roll(s, 2, 0)
                return jnp.concatenate([s * (1.0 / 128)] * 32, axis=0)

            v = v - over_channels(v)
            v = v * lax.rsqrt(over_channels(v * v) + EPS)
            out = dot(v.astype(BF16), w_last[...], 0, 0)
            change = out * gates[third * 12 + q]
            for parity in range(2):
                new = pair_rows(2 * q + parity, third).astype(F32)
                new = (new + change[:, parity * 128 : (parity + 1) * 128]).astype(BF16)
                for b in range(4):
                    updated[b, 2 * q + parity, third * 32 : (third + 1) * 32, :] = new[
                        b * 32 : (b + 1) * 32
                    ]
                total = total + jnp.sum(jnp.abs(new.astype(F32)).reshape(16, 8, 128), axis=0)
            return total

        return steps(count, 3 if count in (3, 9) else U_LAST, lambda n, carry: body(first + n, carry), total)

    def hold(block, own):
        pass

    wait_part(recv_r.at[0])
    multiply(0, hold)
    wait_part(recv_r.at[1])
    send_third(0, 0, 12, recv_t.at[0])
    multiply(1, hold)
    wait_part(recv_r.at[2])
    send_third(1, 0, 12, recv_t.at[1])
    multiply(2, lambda block, own: send_block(2, block, own, 0, 9, recv_t.at[2]))
    send_third(2, 9, 3, recv_t.at[3])
    total = jnp.zeros((8, 128), F32)
    for third in range(2):
        wait_part(recv_t.at[third])
        total = finish(third, 0, 12, total)
    wait_part(recv_t.at[2], 9)
    total = finish(2, 0, 9, total)
    wait_part(recv_t.at[3], 3)
    total = finish(2, 9, 3, total)

    flat = core * 64 + me
    mine = jnp.sum(total, axis=0, keepdims=True)
    s_all[...] = mine
    d_all[flat] = mine
    for _ in range(3):
        wait_part(send_l)
        wait_part(send_r)
        wait_part(send_t)
    pl.semaphore_wait(slab, 1)
    for device in everyone_else:
        pltpu.make_async_remote_copy(
            src_ref=s_all,
            dst_ref=d_all.at[flat],
            send_sem=send_m,
            recv_sem=recv_all,
            device_id=device,
            device_id_type=MESH_ID,
        ).start()
    rest = d_all.at[pl.ds(0, 127)]
    pltpu.make_async_copy(rest, rest, recv_all).wait()
    sums[...] = jnp.sum(d_all.reshape(128, 128)[...].reshape(16, 8, 128), axis=0)
    pltpu.make_async_copy(rest, rest, send_m).wait()


def hand_over(entries, updated, sums, out, total, done):
    copies = [pltpu.make_async_copy(updated.at[b], out.at[b], done.at[b]) for b in range(4)]
    for copy in copies:
        copy.start()
    everyone = jnp.sum(sums[...], axis=0, keepdims=True)
    total[...] = jnp.sum(everyone, axis=1, keepdims=True) * (1.0 / entries)
    for copy in copies:
        copy.wait()


def per_device(entries, pair_repr, seq_lengths, weight_in, weight_out):
    vmem = pl.BlockSpec(memory_space=pltpu.VMEM)
    hbm = pl.BlockSpec(memory_space=pl.ANY)
    dma = pltpu.SemaphoreType.DMA
    updated, sums = pl.pallas_call(
        kernel,
        out_shape=(
            pltpu.VMEM(pair_repr.shape, BF16),
            pltpu.VMEM((8, 128), F32),
        ),
        in_specs=[hbm, hbm, hbm, hbm],
        out_specs=(vmem, vmem),
        scratch_shapes=[
            pltpu.SMEM(seq_lengths.shape, jnp.int32),
            pltpu.VMEM(pair_repr.shape, BF16),
            pltpu.VMEM(weight_in.shape, BF16),
            pltpu.VMEM(weight_out.shape, BF16),
            pltpu.VMEM((36, 128, 2, 128), BF16),
            pltpu.VMEM((36, 128, 2, 128), BF16),
            pltpu.VMEM((2, 3, 4, 192, 2, 128), BF16),
            pltpu.VMEM((2, 3, 4, 192, 2, 128), BF16),
            pltpu.VMEM((8, 384, 384), BF16),
            pltpu.VMEM((2, 384, 512), BF16),
            pltpu.VMEM((3, 64, 12, 4, 128), BF16),
            pltpu.VMEM((36, 256, 128), BF16),
            pltpu.VMEM((36, 128, 256), BF16),
            pltpu.VMEM((36, 128, 256), F32),
            pltpu.VMEM((1024, 256), BF16),
            pltpu.VMEM((256, 256), BF16),
            pltpu.VMEM((256, 256), BF16),
            pltpu.VMEM((1, 128), F32),
            pltpu.VMEM((128, 1, 128), F32),
            dma,
            dma,
            dma,
            dma,
            dma((3,)),
            dma((3,)),
            dma((5,)),
            dma,
            dma((6,)),
            pltpu.SemaphoreType.REGULAR,
        ],
        compiler_params=pltpu.CompilerParams(
            collective_id=0, has_side_effects=True, vmem_limit_bytes=56 * 2**20
        ),
        name="triangle",
    )(seq_lengths, pair_repr, weight_in, weight_out)
    out, total = pl.pallas_call(
        lambda *refs: hand_over(entries, *refs),
        out_shape=(
            jax.ShapeDtypeStruct(pair_repr.shape, BF16),
            jax.ShapeDtypeStruct((1, 1), F32),
        ),
        in_specs=[vmem, vmem],
        out_specs=(hbm, vmem),
        scratch_shapes=[dma((4,))],
        compiler_params=pltpu.CompilerParams(vmem_limit_bytes=2**20),
        name="hand_over",
    )(updated, sums)
    return out, total.reshape(())


def solution(mesh):
    finer = Mesh(mesh.devices.reshape(mesh.shape["gz"], 4, 4, mesh.shape["gy"]), AXES)
    entries = float(8 * 384 * 384 * 128)
    return jax.shard_map(
        lambda *args: per_device(entries, *args),
        mesh=finer,
        in_specs=(P("gz", GX, "gy", None), P(), P(), P()),
        out_specs=(P("gz", GX, "gy", None), P()),
        check_vma=False,
    )
```
